32 devices in a mesh: dp: 8 (over y, x, core), tensor: 4 (over z).
Axes of the slice: x: 2, y: 2, z: 4, core: 2. Of those that a mesh axis runs over, the one named last changes fastest.
Arguments:
- tokens: bfloat16 [8192, 1024], P(('dp', 'tensor')), may hold values from -6 to 6
- segments: int32 [8, 1024], P('dp'), may hold values from 0 to 3, never falling along the last dimension, each value on 1 to 512 neighbouring positions
- w_qkv: bfloat16 [1024, 3, 1024], P(None, None, 'tensor'), may hold values from -0.25 to 0.25
- w_out: bfloat16 [1024, 1024], P('tensor'), may hold values from -1 to 1
- w_up: bfloat16 [1024, 4096], P(None, 'tensor'), may hold values from -0.1875 to 0.1875
- w_down: bfloat16 [4096, 1024], P('tensor'), may hold values from -0.09375 to 0.09375
- gain_one: float32 [1024], replicated, may hold values from 0.5 to 1.5
- shift_one: float32 [1024], replicated, may hold values from -2 to 2
- gain_two: float32 [1024], replicated, may hold values from 0.5 to 1.5
- shift_two: float32 [1024], replicated, may hold values from -2 to 2
- cotangent: bfloat16 [8192, 1024], P(('dp', 'tensor')), may hold values from -6 to 6
Outputs:
- output_rows: bfloat16 [8192, 1024], P(('dp', 'tensor'))
- input_grad: bfloat16 [8192, 1024], P(('dp', 'tensor'))
- grad_qkv: float32 [1024, 3, 1024], P(None, None, 'tensor')
- grad_out: float32 [1024, 1024], P('tensor')
- grad_up: float32 [1024, 4096], P(None, 'tensor')
- grad_down: float32 [4096, 1024], P('tensor')
- grad_gain_one: float32 [1024], replicated
- grad_shift_one: float32 [1024], replicated
- grad_gain_two: float32 [1024], replicated
- grad_shift_two: float32 [1024], replicated
- rms_context: float32 [], replicated
- rms_active: float32 [], replicated
The draws below stay inside these ranges and needn't reach their ends.
Inputs may be any that keep to these rules, and one draw needn't show every extreme that they name: `segments`: within a row (one data group), sequence numbers start at 0, never fall and step by one; each sequence holds 1 to 512 tokens and one holds exactly 512.
All inputs are finite; a program needn't handle non-finite values.
Results may differ from the reference program's by a relative error of at most 0.006.
The reference program's roundings to bfloat16 on the way count: a program that leaves them out, or rounds other values in their place, can miss the bound.
Values may be sent and summed in bfloat16 or wider, within the bound.
A program may use at most 128 MiB of HBM per device.

```python
import math
import jax
import jax.numpy as jnp
import numpy as np
from jax import lax

D = 1024
H = 16
HS = 64
ROT = 16
FF = 4096
GROUP = 1024
SEQS = 4
QBLK = 512
MAXLEN = 512
TOKENS = 8192
N_DP = 8


def block_levels(own_key, dims, cuts, smallest, top_value):
    def one(position, shards_of):
        heights = jax.random.uniform(jax.random.fold_in(jax.random.fold_in(own_key, 6), position), (shards_of,), jnp.float32, smallest / len(cuts), top_value / len(cuts))
        return jnp.repeat(jnp.exp(heights), dims[position] // shards_of).reshape((-1,) + (1,) * (len(dims) - position - 1))

    level = one(*cuts[0])
    for cut in cuts[1:]:
        level = level * one(*cut)
    return level


def profile(amount, total, reach, slope):
    weights = [(1 << 20) // math.isqrt(standing ** slope) + 1 for standing in range(2, amount + 1)]
    spare, given = total - reach - (amount - 1), [1] * (amount - 1)
    while spare > 0:
        candidates = [i for i in range(amount - 1) if given[i] < reach]
        mass, left = sum([weights[i] for i in candidates]), spare
        for i in candidates:
            addition = min(reach - given[i], max(1, left * weights[i] // mass), spare)
            given[i] = given[i] + addition
            spare = spare - addition
    return np.array([reach] + given)


def ragged_sizes(rng, amount, total, reach, lean):
    if amount == 2:
        one = jax.random.randint(rng, (), max(1, total - reach), min(reach, total - 1) + 1)
        return jnp.stack([one, total - one])
    sizes = jnp.asarray(profile(amount, total, reach, lean), jnp.int32)
    couples = (amount - 1) // 2
    source_of, receiver = sizes[1:1 + 2 * couples:2], sizes[2:2 + 2 * couples:2]
    margin = jnp.minimum(source_of - 1, reach - receiver)
    shifted = jax.random.randint(jax.random.fold_in(rng, 1), (couples,), 0, 1 << 20) % (margin + 1)
    sizes = sizes.at[1:1 + 2 * couples:2].set(source_of - shifted).at[2:2 + 2 * couples:2].set(receiver + shifted)
    return sizes[jax.random.permutation(jax.random.fold_in(rng, 2), amount)]


def bell_draw(key, shape, width, limit, shards=(), kind=jnp.bfloat16):
    drawn = width * jax.random.normal(key, shape, jnp.float32)
    if shards:
        drawn = drawn * block_levels(key, shape, shards, -0.22, 0.18)
    return jnp.clip(drawn, -limit, limit).astype(kind)


def setup_inputs(seed: int = 0) -> dict:
    keys = jax.random.split(jax.random.key(seed), 12)
    tokens = bell_draw(keys[0], (TOKENS, D), 1.0, 6.0, ((0, 32),))
    segments = jax.vmap(lambda own: jnp.searchsorted(jnp.cumsum(ragged_sizes(own, SEQS, GROUP, MAXLEN, 1)), jnp.arange(GROUP), side="right"))(jax.random.split(keys[1], N_DP)).reshape((N_DP, GROUP)).astype(jnp.int32)
    w_qkv = bell_draw(keys[2], (D, 3, D), (D // 2) ** -0.5, 0.25, ((2, 4),))
    w_out = bell_draw(keys[3], (D, D), (D // 32) ** -0.5, 1.0, ((0, 4),))
    w_up = bell_draw(keys[4], (D, FF), D ** -0.5, 0.1875, ((1, 4),))
    w_down = bell_draw(keys[5], (FF, D), FF ** -0.5, 0.09375, ((0, 4),))
    gain_one = jnp.clip(1.0 + 0.1 * jax.random.normal(keys[6], (D,), jnp.float32), 0.5, 1.5)
    shift_one = bell_draw(keys[7], (D,), 0.3, 2.0, (), jnp.float32)
    gain_two = jnp.clip(1.0 + 0.1 * jax.random.normal(keys[8], (D,), jnp.float32), 0.5, 1.5)
    shift_two = bell_draw(keys[9], (D,), 0.3, 2.0, (), jnp.float32)
    cotangent = bell_draw(keys[10], (TOKENS, D), 1.0, 6.0, ((0, 32),))
    return {"tokens": tokens, "segments": segments, "w_qkv": w_qkv, "w_out": w_out, "w_up": w_up, "w_down": w_down, "gain_one": gain_one, "shift_one": shift_one, "gain_two": gain_two, "shift_two": shift_two, "cotangent": cotangent}


highest = lax.Precision.HIGHEST
epsilon = 1e-05
rotary_base = 10000.0
masked_score = -1000000000.0

@jax.custom_vjp
def low(v):
    return lax.optimization_barrier(v.astype(jnp.bfloat16)).astype(jnp.float32)

@jax.custom_vjp
def low_back(v):
    return v

def low_keep(v):
    return (low(v), None)

def low_pass(kept, grad):
    return (grad,)

def back_keep(v):
    return (v, None)

def back_low(kept, grad):
    return (low(grad),)
low.defvjp(low_keep, low_pass)
low_back.defvjp(back_keep, back_low)

def layer_norm(values, gain_vector, shift_vector):
    average = lax.optimization_barrier(jnp.mean(values, axis=-1, keepdims=True))
    centred = values - average
    variance = lax.optimization_barrier(jnp.mean(centred * centred, axis=-1, keepdims=True))
    return centred * lax.rsqrt(variance + epsilon) * gain_vector + shift_vector

def seq_positions(seg_row):
    row_index = jnp.arange(seg_row.shape[0], dtype=jnp.int32)
    starts_here = jnp.concatenate([jnp.ones((1,), dtype=bool), seg_row[1:] != seg_row[:-1]])
    seq_start = lax.cummax(jnp.where(starts_here, row_index, 0), axis=0)
    return row_index - seq_start

def rotary_angles(seg_row):
    half_rot = ROT // 2
    frequency = rotary_base ** (-(2.0 * jnp.arange(half_rot, dtype=jnp.float32)) / ROT)
    return seq_positions(seg_row).astype(jnp.float32)[:, None] * frequency[None, :]

def rotate(vectors, angles):
    half_rot = ROT // 2
    shape_rot = (angles.shape[0],) + (1,) * (vectors.ndim - 2) + (half_rot,)
    cosine = jnp.cos(angles).reshape(shape_rot)
    sine_part = jnp.sin(angles).reshape(shape_rot)
    front = vectors[..., :half_rot]
    behind = vectors[..., half_rot:ROT]
    return jnp.concatenate([front * cosine - behind * sine_part, behind * cosine + front * sine_part, vectors[..., ROT:]], axis=-1)

def attend_block(block_queries, keys_all, values_all, seg_row, start):
    query_index = start + jnp.arange(QBLK, dtype=jnp.int32)
    key_index = jnp.arange(seg_row.shape[0], dtype=jnp.int32)
    seg_block = lax.dynamic_slice_in_dim(seg_row, start, QBLK, 0)
    allowed = (seg_block[:, None] == seg_row[None, :]) & (key_index[None, :] <= query_index[:, None])
    scores = low_back(jnp.einsum('qhd,khd->hqk', block_queries, keys_all, precision=highest) * HS ** (-0.5))
    scores = jnp.where(allowed[None], scores, masked_score)
    row_max = lax.optimization_barrier(jnp.max(scores, axis=-1, keepdims=True))
    weights_exp = jnp.exp(scores - row_max)
    weights_soft = low(weights_exp / lax.optimization_barrier(jnp.sum(weights_exp, axis=-1, keepdims=True)))
    return jnp.einsum('hqk,khd->qhd', weights_soft, values_all, precision=highest)

def group_forward(tokens_group, seg_row, w_qkv, w_out, w_up, w_down, gain_one, shift_one, gain_two, shift_two):
    normed_one = low(layer_norm(tokens_group, gain_one, shift_one))
    normed_two = low(layer_norm(tokens_group, gain_two, shift_two))
    projected = low_back(jnp.dot(normed_one, w_qkv.reshape(D, 3 * D), precision=highest)).reshape(GROUP, 3, H, HS)
    angles = rotary_angles(seg_row)
    turned = rotate(projected[:, 0:2], angles)
    queries = low(turned[:, 0])
    keys_all = low(turned[:, 1])
    values_all = low(projected[:, 2])

    def one_block(start):
        block_queries = lax.dynamic_slice_in_dim(queries, start, QBLK, 0)
        return attend_block(block_queries, keys_all, values_all, seg_row, start)
    block_starts = jnp.arange(GROUP // QBLK, dtype=jnp.int32) * QBLK
    context = lax.map(jax.checkpoint(one_block), block_starts).reshape(GROUP, D)
    square_context = jnp.sum(context * context)
    attended = jnp.dot(low(low_back(context)), w_out, precision=highest)
    hidden = low_back(jnp.dot(normed_two, w_up, precision=highest))
    activated = jax.nn.gelu(hidden, approximate=False)
    square_active = jnp.sum(activated * activated)
    mixed = jnp.dot(low(activated), w_down, precision=highest)
    return (tokens_group + attended + mixed, (square_context, square_active))

def reference(tokens, segments, w_qkv, w_out, w_up, w_down, gain_one, shift_one, gain_two, shift_two, cotangent):
    weights = (w_qkv.astype(jnp.float32), w_out.astype(jnp.float32), w_up.astype(jnp.float32), w_down.astype(jnp.float32), gain_one, shift_one, gain_two, shift_two)
    tokens_all = tokens.astype(jnp.float32).reshape(N_DP, GROUP, D)
    checked = jax.checkpoint(group_forward)

    def whole_layer(tokens_in, wq, wo, wu, wd, ga, sa, gb, sb):

        def scan_step(running, item):
            tokens_group, seg_row = item
            result, squares = checked(tokens_group, seg_row, wq, wo, wu, wd, ga, sa, gb, sb)
            return ((running[0] + squares[0], running[1] + squares[1]), result)
        start_sums = (jnp.zeros((), jnp.float32), jnp.zeros((), jnp.float32))
        sums, results = lax.scan(scan_step, start_sums, (tokens_in, segments))
        return (results, sums)
    results, pullback, sums = jax.vjp(whole_layer, tokens_all, *weights, has_aux=True)
    grads = pullback(cotangent.astype(jnp.float32).reshape(N_DP, GROUP, D))
    output_rows = results.reshape(TOKENS, D).astype(jnp.bfloat16)
    input_grad = grads[0].reshape(TOKENS, D).astype(jnp.bfloat16)
    rms_context = jnp.sqrt(sums[0] / (TOKENS * D))
    rms_active = jnp.sqrt(sums[1] / (TOKENS * FF))
    return (output_rows, input_grad, grads[1], grads[2], grads[3], grads[4], grads[5], grads[6], grads[7], grads[8], rms_context, rms_active)
```

```python
from functools import partial

import jax
import jax.numpy as jnp
from jax import lax
from jax.sharding import PartitionSpec as P

HS = 64
ROT = 16
FF = 4096
QBLK = 512


epsilon = 1e-05
rotary_base = 10000.0
masked_score = -1000000000.0


def layer_norm(values, gain_vector, shift_vector):
    average = jnp.mean(values, axis=-1, keepdims=True)
    centred = values - average
    variance = jnp.mean(centred * centred, axis=-1, keepdims=True)
    return centred * lax.rsqrt(variance + epsilon) * gain_vector + shift_vector


def unit_rows(values):
    average = jnp.mean(values, axis=-1, keepdims=True)
    centred = values - average
    variance = jnp.mean(centred * centred, axis=-1, keepdims=True)
    scale = lax.rsqrt(variance + epsilon)
    return centred * scale, scale


def exact_gelu(values):
    return jax.nn.gelu(values, approximate=False)


def seq_positions(seg_row):
    row_index = jnp.arange(seg_row.shape[0], dtype=jnp.int32)
    starts_here = jnp.concatenate([jnp.ones((1,), dtype=bool), seg_row[1:] != seg_row[:-1]])
    seq_start = lax.cummax(jnp.where(starts_here, row_index, 0), axis=0)
    return row_index - seq_start


def rotary_angles(seg_row):
    half_rot = ROT // 2
    frequency = rotary_base ** (-(2.0 * jnp.arange(half_rot, dtype=jnp.float32)) / ROT)
    return seq_positions(seg_row).astype(jnp.float32)[:, None] * frequency[None, :]


def rotate(vectors, angles):
    half_rot = ROT // 2
    shape_rot = (angles.shape[0],) + (1,) * (vectors.ndim - 2) + (half_rot,)
    cosine = jnp.cos(angles).reshape(shape_rot)
    sine_part = jnp.sin(angles).reshape(shape_rot)
    front = vectors[..., :half_rot]
    behind = vectors[..., half_rot:ROT]
    return jnp.concatenate(
        [
            front * cosine - behind * sine_part,
            behind * cosine + front * sine_part,
            vectors[..., ROT:],
        ],
        axis=-1,
    )


def masked_scores(block_queries, keys_all, seg_row, start):
    query_index = start + jnp.arange(QBLK, dtype=jnp.int32)
    key_index = jnp.arange(seg_row.shape[0], dtype=jnp.int32)
    seg_block = lax.dynamic_slice_in_dim(seg_row, start, QBLK, 0)
    allowed = (seg_block[:, None] == seg_row[None, :]) & (
        key_index[None, :] <= query_index[:, None]
    )
    scores = jnp.einsum(
        "qhd,khd->hqk", block_queries, keys_all, preferred_element_type=jnp.float32
    ) * HS ** (-0.5)
    return jnp.where(allowed[None], scores, masked_score)


def per_device(
    tokens,
    segments,
    w_qkv,
    w_out,
    w_up,
    w_down,
    gain_one,
    shift_one,
    gain_two,
    shift_two,
    cotangent,
):
    seg_row = segments[0]
    group = seg_row.shape[0]
    width = tokens.shape[1]
    local_width = w_qkv.shape[2]
    heads_local = local_width // HS
    block_starts = jnp.arange(group // QBLK, dtype=jnp.int32) * QBLK
    tokens_own = tokens.astype(jnp.float32)
    cotangent_own = cotangent.astype(jnp.float32)
    tokens_all = lax.all_gather(tokens, "tensor", axis=0, tiled=True).astype(jnp.float32)
    unit_all, _ = unit_rows(tokens_all)
    normed_one = (unit_all * gain_one + shift_one).astype(jnp.bfloat16)
    normed_two = (unit_all * gain_two + shift_two).astype(jnp.bfloat16)
    qkv_matrix = w_qkv.reshape(width, 3 * local_width)
    projected = jnp.dot(normed_one, qkv_matrix, preferred_element_type=jnp.float32).reshape(
        group, 3, heads_local, HS
    )
    angles = rotary_angles(seg_row)
    turned = rotate(projected[:, 0:2], angles).astype(jnp.bfloat16)
    queries = turned[:, 0]
    keys_all = turned[:, 1]
    values_all = projected[:, 2].astype(jnp.bfloat16)

    def forward_block(start):
        block_queries = lax.dynamic_slice_in_dim(queries, start, QBLK, 0)
        scores = masked_scores(block_queries, keys_all, seg_row, start)
        row_max = jnp.max(scores, axis=-1, keepdims=True)
        weights_exp = jnp.exp(scores - row_max)
        total_exp = jnp.sum(weights_exp, axis=-1, keepdims=True)
        weights_soft = (weights_exp / total_exp).astype(jnp.bfloat16)
        block_context = jnp.einsum(
            "hqk,khd->qhd", weights_soft, values_all, preferred_element_type=jnp.float32
        )
        return (block_context, (row_max + jnp.log(total_exp))[..., 0])

    context_blocks, log_totals = lax.map(forward_block, block_starts)
    context = context_blocks.reshape(group, local_width)
    square_context = jnp.sum(context * context)
    context_low = context.astype(jnp.bfloat16)
    hidden = jnp.dot(normed_two, w_up, preferred_element_type=jnp.float32)
    activated, gelu_back = jax.vjp(exact_gelu, hidden)
    square_active = jnp.sum(activated * activated)
    active_low = activated.astype(jnp.bfloat16)
    partial_rows = jnp.dot(context_low, w_out, preferred_element_type=jnp.float32) + jnp.dot(
        active_low, w_down, preferred_element_type=jnp.float32
    )
    branch = lax.psum_scatter(
        partial_rows.astype(jnp.bfloat16), "tensor", scatter_dimension=0, tiled=True
    ).astype(jnp.float32)
    output_rows = (tokens_own + branch).astype(jnp.bfloat16)
    cotangent_all = lax.all_gather(cotangent, "tensor", axis=0, tiled=True)
    grad_down = jnp.einsum(
        "tf,td->fd", active_low, cotangent_all, preferred_element_type=jnp.float32
    )
    grad_active = jnp.einsum("td,fd->tf", cotangent_all, w_down, preferred_element_type=jnp.float32)
    grad_hidden = gelu_back(grad_active)[0].astype(jnp.bfloat16)
    grad_up = jnp.einsum("td,tf->df", normed_two, grad_hidden, preferred_element_type=jnp.float32)
    grad_normed_two = jnp.einsum("tf,df->td", grad_hidden, w_up, preferred_element_type=jnp.float32)
    grad_out = jnp.einsum(
        "tc,td->cd", context_low, cotangent_all, preferred_element_type=jnp.float32
    )
    grad_context = (
        jnp.einsum("td,cd->tc", cotangent_all, w_out, preferred_element_type=jnp.float32)
        .astype(jnp.bfloat16)
        .reshape(group, heads_local, HS)
    )
    score_scale = HS ** (-0.5)

    def backward_block(running, item):
        start, log_total = item
        grad_keys, grad_values = running
        block_queries = lax.dynamic_slice_in_dim(queries, start, QBLK, 0)
        block_grad = lax.dynamic_slice_in_dim(grad_context, start, QBLK, 0)
        scores = masked_scores(block_queries, keys_all, seg_row, start)
        weights_soft = jnp.exp(scores - log_total[..., None])
        weights_low = weights_soft.astype(jnp.bfloat16)
        grad_values = grad_values + jnp.einsum(
            "hqk,qhd->khd", weights_low, block_grad, preferred_element_type=jnp.float32
        )
        grad_weights = jnp.einsum(
            "qhd,khd->hqk", block_grad, values_all, preferred_element_type=jnp.float32
        )
        inner_sum = jnp.sum(weights_soft * grad_weights, axis=-1, keepdims=True)
        grad_scores = (weights_soft * (grad_weights - inner_sum)).astype(jnp.bfloat16)
        grad_block_queries = (
            jnp.einsum("hqk,khd->qhd", grad_scores, keys_all, preferred_element_type=jnp.float32)
            * score_scale
        )
        grad_keys = (
            grad_keys
            + jnp.einsum(
                "hqk,qhd->khd", grad_scores, block_queries, preferred_element_type=jnp.float32
            )
            * score_scale
        )
        return ((grad_keys, grad_values), grad_block_queries)

    zero_heads = jnp.zeros((group, heads_local, HS), jnp.float32)
    (grad_keys, grad_values), grad_query_blocks = lax.scan(
        backward_block, (zero_heads, zero_heads), (block_starts, log_totals)
    )
    grad_queries = grad_query_blocks.reshape(group, heads_local, HS)
    _, rotate_back = jax.vjp(partial(rotate, angles=angles), projected[:, 0:2])
    grad_turned = rotate_back(jnp.stack([grad_queries, grad_keys], axis=1))[0]
    grad_projected = (
        jnp.concatenate([grad_turned, grad_values[:, None]], axis=1)
        .astype(jnp.bfloat16)
        .reshape(group, 3 * local_width)
    )
    grad_qkv = jnp.einsum(
        "td,tc->dc", normed_one, grad_projected, preferred_element_type=jnp.float32
    ).reshape(width, 3, local_width)
    grad_normed_one = jnp.einsum(
        "tc,dc->td", grad_projected, qkv_matrix, preferred_element_type=jnp.float32
    )
    grad_qkv, grad_out, grad_up, grad_down = (
        summed.astype(jnp.float32)
        for summed in lax.psum(
            tuple(g.astype(jnp.bfloat16) for g in (grad_qkv, grad_out, grad_up, grad_down)), "dp"
        )
    )
    grad_gain_one = jnp.sum(grad_normed_one * unit_all, axis=0)
    grad_shift_one = jnp.sum(grad_normed_one, axis=0)
    grad_gain_two = jnp.sum(grad_normed_two * unit_all, axis=0)
    grad_shift_two = jnp.sum(grad_normed_two, axis=0)
    weighted = grad_normed_one * gain_one + grad_normed_two * gain_two
    weighted = lax.psum_scatter(
        weighted.astype(jnp.bfloat16), "tensor", scatter_dimension=0, tiled=True
    ).astype(jnp.float32)
    unit_own, scale_own = unit_rows(tokens_own)
    grad_input_rows = scale_own * (
        weighted
        - jnp.mean(weighted, axis=-1, keepdims=True)
        - unit_own * jnp.mean(weighted * unit_own, axis=-1, keepdims=True)
    )
    input_grad = (cotangent_own + grad_input_rows).astype(jnp.bfloat16)
    totals = lax.psum(
        (
            grad_gain_one,
            grad_shift_one,
            grad_gain_two,
            grad_shift_two,
            square_context,
            square_active,
        ),
        ("dp", "tensor"),
    )
    token_count = group * lax.axis_size("dp")
    rms_context = jnp.sqrt(totals[4] / (token_count * width))
    rms_active = jnp.sqrt(totals[5] / (token_count * FF))
    return (
        output_rows,
        input_grad,
        grad_qkv,
        grad_out,
        grad_up,
        grad_down,
        totals[0],
        totals[1],
        totals[2],
        totals[3],
        rms_context,
        rms_active,
    )


def solution(mesh):
    return jax.shard_map(
        per_device,
        mesh=mesh,
        in_specs=(
            P(("dp", "tensor"), None),
            P("dp", None),
            P(None, None, "tensor"),
            P("tensor", None),
            P(None, "tensor"),
            P("tensor", None),
            P(),
            P(),
            P(),
            P(),
            P(("dp", "tensor"), None),
        ),
        out_specs=(
            P(("dp", "tensor"), None),
            P(("dp", "tensor"), None),
            P(None, None, "tensor"),
            P("tensor", None),
            P(None, "tensor"),
            P("tensor", None),
            P(),
            P(),
            P(),
            P(),
            P(),
            P(),
        ),
        check_vma=False,
    )
```

```python
from functools import partial, reduce

import jax
import jax.numpy as jnp
from jax import lax
from jax.experimental import pallas as pl
from jax.experimental.pallas import tpu as pltpu
from jax.sharding import PartitionSpec as P

HS = 64
ROT = 16
FF = 4096
BLOCK = 256
LONGEST = 512
LANES = 128

epsilon = 1e-05
rotary_base = 10000.0
masked_score = -1000000000.0
low = jnp.bfloat16
full = jnp.float32
MESH = pl.DeviceIdType.MESH


def dot(a, b, over_a, over_b):
    return lax.dot_general(
        a, b, (((over_a,), (over_b,)), ((), ())), preferred_element_type=jnp.float32
    )


def total(parts):
    return reduce(jnp.add, parts)


def unit_rows(values):
    average = jnp.mean(values, axis=-1, keepdims=True)
    centred = values - average
    variance = jnp.mean(centred * centred, axis=-1, keepdims=True)
    scale = lax.rsqrt(variance + epsilon)
    return centred * scale, scale


def block_rows(index):
    return slice(index * BLOCK, (index + 1) * BLOCK)


def key_blocks(index):
    reach = (LONGEST + BLOCK - 2) // BLOCK
    return range(max(0, index - reach), index + 1)


def scores_turned(query, keys, seg_col, seg_row, head, at, key_at):
    scores = dot(keys[head, block_rows(key_at), :], query, 1, 1) * HS ** (-0.5)
    allowed = seg_col[block_rows(key_at), :] == seg_row[:, block_rows(at)]
    if at == key_at:
        key_index = lax.broadcasted_iota(jnp.int32, (BLOCK, BLOCK), 0)
        query_index = lax.broadcasted_iota(jnp.int32, (BLOCK, BLOCK), 1)
        allowed = allowed & (key_index <= query_index)
    return jnp.where(allowed, scores, masked_score)


def remote(source, target, send, receive, **device):
    return pltpu.make_async_remote_copy(
        source, target, send, receive, device_id=device, device_id_type=MESH
    )


class DataSum:
    def __init__(self, spots, bufs, send, receive):
        self.part, self.done, self.half, self.a1, self.b1, self.a2, self.b2 = bufs
        self.core, self.x, self.y, self.nx = spots
        self.send, self.receive = send, receive
        rows = self.part.shape[0]
        self.rows = rows
        self.open = []

    def dp(self, core=None, x=None, y=None):
        core = self.core if core is None else core
        x = self.x if x is None else x
        y = self.y if y is None else y
        return (y * self.nx + x) * 2 + core

    def rows_at(self, start, size):
        return pl.ds(pl.multiple_of(start, size), size)

    def put(self, source, target, base, mine, peer, device):
        copy = remote(
            source, target, self.send.at[base + peer], self.receive.at[base + mine], dp=device
        )
        copy.start()
        self.open.append(copy)

    def take(self, target, base, peer):
        remote(
            target, target, self.send.at[base + peer], self.receive.at[base + peer],
            dp=self.dp(),
        ).wait_recv()

    def drain(self):
        for copy in self.open:
            copy.wait_send()
        self.open = []

    def x_peers(self):
        return [lax.rem(self.x + step, self.nx) for step in range(1, self.nx)]

    def bases(self):
        nx = self.nx
        names = {}
        at = 0
        for name, size in (
            ("c", 2), ("a1", nx), ("b1", 2), ("a2", 2), ("b2", nx),
            ("a3", 2), ("b3", nx), ("a4", nx), ("b4", 2), ("d", 2),
        ):
            names[name] = at
            at += size
        names["all"] = at
        return names

    def stage(self, number):
        rows, nx, core, x, y = self.rows, self.nx, self.core, self.x, self.y
        base = self.bases()
        half, quarter, eighth = rows // 2, rows // 4, rows // 8
        a_size, b_size, tail = quarter // nx, eighth, eighth // nx
        other, across = 1 - core, 1 - y
        start = core * half
        if number == 0:
            self.put(
                self.part.at[self.rows_at(other * half, half), :], self.half,
                base["c"], core, other, self.dp(core=other),
            )
        if number == 1:
            self.take(self.half, base["c"], other)
            add_rows(
                self.half, 0, [(self.part, start), (self.half, 0)], half
            )
            self.drain()
            for peer in self.x_peers():
                self.put(
                    self.half.at[self.rows_at(peer * a_size, a_size), :], self.a1.at[x],
                    base["a1"], x, peer, self.dp(x=peer),
                )
            self.put(
                self.half.at[self.rows_at(quarter + across * b_size, b_size), :], self.b1.at[y],
                base["b1"], y, across, self.dp(y=across),
            )
        if number == 2:
            for peer in self.x_peers():
                self.take(self.a1.at[peer], base["a1"], peer)
            add_rows(
                self.half, x * a_size,
                [(self.half, x * a_size)] + [(self.a1.at[peer], 0) for peer in self.x_peers()],
                a_size,
            )
            self.take(self.b1.at[across], base["b1"], across)
            add_rows(
                self.half, quarter + y * b_size,
                [(self.half, quarter + y * b_size), (self.b1.at[across], 0)],
                b_size,
            )
            self.drain()
            self.put(
                self.half.at[self.rows_at(x * a_size + across * tail, tail), :], self.a2.at[y],
                base["a2"], y, across, self.dp(y=across),
            )
            for peer in self.x_peers():
                self.put(
                    self.half.at[self.rows_at(quarter + y * b_size + peer * tail, tail), :],
                    self.b2.at[x], base["b2"], x, peer, self.dp(x=peer),
                )
        if number == 3:
            a_own = x * a_size + y * tail
            b_own = quarter + y * b_size + x * tail
            self.take(self.a2.at[across], base["a2"], across)
            add_rows(
                self.done, start + a_own, [(self.half, a_own), (self.a2.at[across], 0)], tail
            )
            for peer in self.x_peers():
                self.take(self.b2.at[peer], base["b2"], peer)
            add_rows(
                self.done, start + b_own,
                [(self.half, b_own)] + [(self.b2.at[peer], 0) for peer in self.x_peers()],
                tail,
            )
            self.drain()
            piece = self.done.at[self.rows_at(start + a_own, tail), :]
            self.put(piece, piece, base["a3"], y, across, self.dp(y=across))
            piece = self.done.at[self.rows_at(start + b_own, tail), :]
            for peer in self.x_peers():
                self.put(piece, piece, base["b3"], x, peer, self.dp(x=peer))
        if number == 4:
            self.take(
                self.done.at[self.rows_at(start + x * a_size + across * tail, tail), :],
                base["a3"], across,
            )
            for peer in self.x_peers():
                self.take(
                    self.done.at[
                        self.rows_at(start + quarter + y * b_size + peer * tail, tail), :
                    ],
                    base["b3"], peer,
                )
            self.drain()
            piece = self.done.at[self.rows_at(start + x * a_size, a_size), :]
            for peer in self.x_peers():
                self.put(piece, piece, base["a4"], x, peer, self.dp(x=peer))
            piece = self.done.at[self.rows_at(start + quarter + y * b_size, b_size), :]
            self.put(piece, piece, base["b4"], y, across, self.dp(y=across))
        if number == 5:
            for peer in self.x_peers():
                self.take(
                    self.done.at[self.rows_at(start + peer * a_size, a_size), :],
                    base["a4"], peer,
                )
            self.take(
                self.done.at[self.rows_at(start + quarter + across * b_size, b_size), :],
                base["b4"], across,
            )
            self.drain()
            piece = self.done.at[self.rows_at(start, half), :]
            self.put(piece, piece, base["d"], core, other, self.dp(core=other))
        if number == 6:
            self.take(self.done.at[self.rows_at(other * half, half), :], base["d"], other)
            self.drain()


def add_rows(target, target_start, sources, size):
    step = min(size, 64)

    def one(index, carry):
        offset = index * step

        def rows(start):
            return pl.ds(pl.multiple_of(start + offset, min(step, 16)), step)

        summed = total([ref[rows(start), :].astype(full) for ref, start in sources])
        target[rows(target_start), :] = summed.astype(target.dtype)
        return carry

    lax.fori_loop(0, size // step, one, 0)


def layer_kernel(
    ring,
    ranks,
    tokens, cotangent, seg_col, seg_row, norms, w_qkv, w_out, w_up, w_down,
    output_rows, input_grad, grad_down_out, grad_up_out, grad_mix_out, vectors_out,
    wq, wo, wu, wd, weight_sem, out_sem,
    x_all, g_all, normed_one, normed_two, active, slope, u_all,
    acc_down, acc_up, queries, keys, values, grad_context, context, logs,
    grad_q, turn_cos, turn_sin,
    gather_send, gather_recv,
    branch_buf, branch_send, branch_recv, grad_buf, grad_send, grad_recv,
    part0, done0, half0, a10, b10, a20, b20,
    done1, half1, a11, b11, a21, b21,
    data_send, data_recv,
    vectors, vec_tensor, vec_core, vec_x, vec_y, vec_send, vec_recv,
):
    group = x_all.shape[0]
    width = x_all.shape[1]
    shard = group // ring
    heads = queries.shape[0]
    local = heads * HS
    blocks = group // BLOCK
    hidden_local = wu.shape[1]
    nx = ranks // 4
    part1 = wu
    grad_proj = normed_two
    t = lax.axis_index("tensor")
    dp = lax.axis_index("dp")
    core = lax.rem(dp, 2)
    x_at = lax.rem(dp // 2, nx)
    y_at = dp // (2 * nx)
    spots = (core, x_at, y_at, nx)

    def rows(s):
        return pl.ds(pl.multiple_of(s * shard, shard), shard)

    def dp_of(c, x, y):
        return (y * nx + x) * 2 + c

    weights = [
        pltpu.make_async_copy(source, target, weight_sem.at[index])
        for index, (source, target) in enumerate(
            ((w_qkv, wq), (w_up, wu), (w_out, wo), (w_down, wd))
        )
    ]
    for copy in weights:
        copy.start()

    barrier = pltpu.get_barrier_semaphore()
    peers = [dict(tensor=lax.rem(t + step, ring)) for step in range(1, ring)]
    peers.append(dict(dp=dp_of(1 - core, x_at, y_at)))
    peers.append(dict(dp=dp_of(core, x_at, 1 - y_at)))
    for step in range(1, nx):
        peers.append(dict(dp=dp_of(core, lax.rem(x_at + step, nx), y_at)))
    for peer in peers:
        pl.semaphore_signal(barrier, inc=1, device_id=peer, device_id_type=MESH)
    pl.semaphore_wait(barrier, len(peers))

    def relay(which, source, s, side):
        target = (x_all, g_all)[which].at[rows(s), :]
        return remote(
            source,
            target,
            gather_send.at[which, side, s],
            gather_recv.at[which, s],
            tensor=t + 1 if side == 0 else t - 1,
        )

    def arrive(which, s):
        target = (x_all, g_all)[which].at[rows(s), :]
        remote(
            target, target, gather_send.at[which, 0, s], gather_recv.at[which, s], tensor=t
        ).wait_recv()

    def gather_step(which, k):
        array = (x_all, g_all)[which]

        @pl.when((k > 0) & (t - k >= 0))
        def _():
            s = t - k
            arrive(which, s)

            @pl.when(t < ring - 1)
            def _():
                relay(which, array.at[rows(s), :], s, 0).start()

        @pl.when((k > 0) & (t + k < ring))
        def _():
            s = t + k
            arrive(which, s)

            @pl.when(t > 0)
            def _():
                relay(which, array.at[rows(s), :], s, 1).start()

    def gather_own(which, side):
        relay(which, (tokens, cotangent)[which], t, side).start()

    def gather_drain(which):
        array = (x_all, g_all)[which]

        def one(s, carry):
            @pl.when((s <= t) & (t < ring - 1))
            def _():
                relay(which, array.at[rows(s), :], s, 0).wait_send()

            @pl.when((s >= t) & (t > 0))
            def _():
                relay(which, array.at[rows(s), :], s, 1).wait_send()

            return carry

        lax.fori_loop(0, ring, one, 0)

    @pl.when(t < ring - 1)
    def _():
        gather_own(0, 0)

    @pl.when(t > 0)
    def _():
        gather_own(0, 1)

    x_all[rows(t), :] = tokens[...]
    g_all[rows(t), :] = cotangent[...]
    vectors[...] = jnp.zeros_like(vectors)
    acc_down[...] = jnp.zeros_like(acc_down)
    acc_up[...] = jnp.zeros_like(acc_up)
    gain_one, shift_one = norms[0:1, :], norms[1:2, :]
    gain_two, shift_two = norms[2:3, :], norms[3:4, :]
    for copy in weights:
        copy.wait()

    lane = lax.broadcasted_iota(jnp.int32, (shard, LANES), 1) % HS

    def turned(part, cosine, sine):
        moved = jnp.where(
            lane < ROT // 2, pltpu.roll(part, LANES - ROT // 2, 1), pltpu.roll(part, ROT // 2, 1)
        )
        return part * cosine + moved * sine

    def forward_rows(s):
        at = rows(s)
        unit, _ = unit_rows(x_all[at, :].astype(full))
        one = (unit * gain_one + shift_one).astype(low)
        two = (unit * gain_two + shift_two).astype(low)
        normed_one[at, :] = one
        normed_two[at, :] = two
        own_segments = seg_col[at, :]
        before = jnp.sum((seg_row[...] < own_segments).astype(jnp.int32), axis=1, keepdims=True)
        index = lax.broadcasted_iota(jnp.int32, (shard, 1), 0) + s * shard
        position = (index - before).astype(full)
        angle = position * norms[4:5, 0:LANES]
        cosine = jnp.cos(angle)
        sine = jnp.sin(angle) * norms[5:6, 0:LANES]
        turn_cos[at, :] = cosine
        turn_sin[at, :] = sine
        projected = dot(one, wq[...], 1, 0)
        for index_part, ref in enumerate((queries, keys, values)):
            for pair in range(local // LANES):
                lo = index_part * local + pair * LANES
                part = projected[:, lo : lo + LANES]
                if index_part < 2:
                    part = turned(part, cosine, sine)
                part = part.astype(low)
                for side in range(LANES // HS):
                    ref[pair * (LANES // HS) + side, at, :] = part[:, side * HS : (side + 1) * HS]
        hidden = dot(two, wu[...], 1, 0)
        inner = 0.5 * (1.0 + lax.erf(hidden * 0.7071067811865476))
        activated = hidden * inner
        steep = inner + hidden * jnp.exp(-0.5 * hidden * hidden) * 0.3989422804014327
        active[at, :] = activated.astype(low)
        for chunk in range(hidden_local // LANES):
            slope[chunk, at, :] = steep[:, chunk * LANES : (chunk + 1) * LANES]
        vectors[4:5, 0:hidden_local] += jnp.sum(activated * activated, axis=0, keepdims=True)

    def both_sides(k, body):
        def one(side, carry):
            s = jnp.where(side == 0, t - k, t + k)

            @pl.when((s >= 0) & (s < ring) & ((k > 0) | (side == 0)))
            def _():
                body(s)

            return carry

        lax.fori_loop(0, 2, one, 0)

    def forward_step(k, carry):
        gather_step(0, k)

        @pl.when((k == t) & (t < ring - 1))
        def _():
            gather_own(1, 0)

        @pl.when((k == ring - 1 - t) & (t > 0))
        def _():
            gather_own(1, 1)

        both_sides(k, forward_rows)
        return carry

    lax.fori_loop(0, ring, forward_step, 0)

    for at in range(blocks):

        def forward_head(head, carry, at=at):
            query = queries[head, block_rows(at), :]
            spans = key_blocks(at)
            scores = [
                scores_turned(query, keys, seg_col, seg_row, head, at, span) for span in spans
            ]
            most = reduce(jnp.maximum, [jnp.max(s, axis=0, keepdims=True) for s in scores])
            raised = [jnp.exp(s - most) for s in scores]
            summed = total([jnp.sum(e, axis=0, keepdims=True) for e in raised])
            share = 1.0 / summed
            logs[head, :, block_rows(at)] = most + jnp.log(summed)
            mixed = total(
                [
                    dot((e * share).astype(low), values[head, block_rows(span), :], 0, 0)
                    for e, span in zip(raised, spans)
                ]
            )
            context[head, block_rows(at), :] = mixed.astype(low)
            vectors[5:6, 0:HS] += jnp.sum(mixed * mixed, axis=0, keepdims=True)
            return carry

        lax.fori_loop(0, heads, forward_head, 0)

    def heads_side_by_side(ref, at):
        return jnp.concatenate([ref[head, at, :] for head in range(heads)], axis=1)

    def branch_rows(s):
        at = rows(s)
        return dot(heads_side_by_side(context, at), wo[...], 1, 0) + dot(
            active[at, :], wd[...], 1, 0
        )

    def chain(buffer, send, receive, make):
        def hop(s, side):
            if side == 0:
                slot = s
            else:
                slot = jnp.where(s == t - 1, ring, s)
            return remote(
                buffer.at[s],
                buffer.at[slot],
                send.at[s],
                receive.at[slot],
                tensor=t + 1 if side == 0 else t - 1,
            )

        def landed(slot):
            remote(buffer.at[slot], buffer.at[slot], send.at[0], receive.at[slot], tensor=t).wait_recv()

        def pass_on(s, side):
            has = t > 0 if side == 0 else t < ring - 1

            @pl.when(has)
            def _():
                landed(s)
                buffer[s] = (make(s) + buffer[s].astype(full)).astype(low)

            @pl.when(jnp.logical_not(has))
            def _():
                buffer[s] = make(s).astype(low)

            hop(s, side).start()

        def own():
            value = make(t)
            carried = [value]

            @pl.when(t > 0)
            def _():
                landed(t)

            @pl.when(t < ring - 1)
            def _():
                landed(ring)

            left = jnp.where(t > 0, buffer[t].astype(full), 0.0)
            right = jnp.where(t < ring - 1, buffer[ring].astype(full), 0.0)
            return value + left + right

        def drain():
            def one(s, carry):
                @pl.when(s > t)
                def _():
                    hop(s, 0).wait_send()

                @pl.when(s < t)
                def _():
                    hop(s, 1).wait_send()

                return carry

            lax.fori_loop(0, ring, one, 0)

        return pass_on, own, drain

    branch_pass, branch_own, branch_drain = chain(
        branch_buf, branch_send, branch_recv, branch_rows
    )

    def backward_rows(s):
        at = rows(s)
        grad = g_all[at, :]
        grad_active = dot(grad, wd[...], 1, 1)
        steep = jnp.concatenate(
            [slope[chunk, at, :] for chunk in range(hidden_local // LANES)], axis=1
        )
        grad_hidden = (grad_active * steep).astype(low)
        for block in range(hidden_local // BLOCK):
            acc_down[block_rows(block), :] += dot(active[at, block_rows(block)], grad, 0, 0)
        for block in range(width // BLOCK):
            acc_up[block_rows(block), :] += dot(
                normed_two[at, block_rows(block)], grad_hidden, 0, 0
            )
        grad_two = dot(grad_hidden, wu[...], 1, 1)
        unit, _ = unit_rows(x_all[at, :].astype(full))
        vectors[2:3, 0:width] += jnp.sum(grad_two * unit, axis=0, keepdims=True)
        vectors[3:4, 0:width] += jnp.sum(grad_two, axis=0, keepdims=True)
        u_all[at, :] = grad_two * gain_two
        back = dot(grad, wo[...], 1, 1).astype(low)
        for head in range(heads):
            grad_context[head, at, :] = back[:, head * HS : (head + 1) * HS]

    def backward_step(k, carry):
        gather_step(1, k)

        s_up = ring - 1 - k + t

        @pl.when((s_up > t) & (s_up < ring))
        def _():
            branch_pass(s_up, 0)

        s_down = k - (ring - 1 - t)

        @pl.when((s_down >= 0) & (s_down < t))
        def _():
            branch_pass(s_down, 1)

        both_sides(k, backward_rows)
        return carry

    lax.fori_loop(0, ring, backward_step, 0)

    def narrow(source, target):
        step = 64

        def one(index, carry):
            at = pl.ds(pl.multiple_of(index * step, step), step)
            target[at, :] = source[at, :].astype(low)
            return carry

        lax.fori_loop(0, source.shape[0] // step, one, 0)

    down_sum = DataSum(
        spots, (part0, done0, half0, a10, b10, a20, b20), data_send.at[0], data_recv.at[0]
    )
    up_sum = DataSum(
        spots, (part1, done1, half1, a11, b11, a21, b21), data_send.at[1], data_recv.at[1]
    )
    narrow(acc_down, part0)
    down_sum.stage(0)
    narrow(acc_up, part1)
    up_sum.stage(0)

    output_rows[...] = (tokens[...].astype(full) + branch_own()).astype(low)

    def u_rows(s):
        return u_all[rows(s), :]

    grad_pass, grad_own, grad_drain = chain(grad_buf, grad_send, grad_recv, u_rows)

    def grad_chain_step(j):
        s_up = ring - 1 - j + t

        @pl.when((s_up > t) & (s_up < ring))
        def _():
            grad_pass(s_up, 0)

        s_down = 2 * (ring - 1) - t - j

        @pl.when((s_down >= 0) & (s_down < t))
        def _():
            grad_pass(s_down, 1)

    grad_keys = slope
    slots = [
        lambda: (down_sum.stage(1), up_sum.stage(1)),
        lambda: (down_sum.stage(2),),
        lambda: (up_sum.stage(2), down_sum.stage(3)),
        lambda: (up_sum.stage(3), down_sum.stage(4)),
    ]
    step_done = 0
    for at in reversed(range(blocks)):

        def backward_head(head, carry, at=at):
            query = queries[head, block_rows(at), :]
            grad = grad_context[head, block_rows(at), :]
            spans = key_blocks(at)
            log_total = logs[head, :, block_rows(at)]
            probs = [
                jnp.exp(
                    scores_turned(query, keys, seg_col, seg_row, head, at, span) - log_total
                )
                for span in spans
            ]
            grad_probs = [dot(values[head, block_rows(span), :], grad, 1, 1) for span in spans]
            inner = total(
                [jnp.sum(p * d, axis=0, keepdims=True) for p, d in zip(probs, grad_probs)]
            )
            grad_query = []
            for p, d, span in zip(probs, grad_probs, spans):
                grad_scores = (p * (d - inner)).astype(low)
                grad_value = dot(p.astype(low), grad, 1, 0)
                grad_key = dot(grad_scores, query, 1, 0) * HS ** (-0.5)
                grad_query.append(dot(grad_scores, keys[head, block_rows(span), :], 0, 0))
                if at == min(span + len(key_blocks(blocks)) - 1, blocks - 1):
                    grad_keys[2 * head, block_rows(span), 0:HS] = grad_key
                    grad_keys[2 * head + 1, block_rows(span), 0:HS] = grad_value
                else:
                    grad_keys[2 * head, block_rows(span), 0:HS] += grad_key
                    grad_keys[2 * head + 1, block_rows(span), 0:HS] += grad_value
            grad_q[head] = total(grad_query) * HS ** (-0.5)
            return carry

        lax.fori_loop(0, heads, backward_head, 0)

        per_block = BLOCK // shard
        for piece in reversed(range(per_block)):
            s = at * per_block + piece
            at_rows = slice(s * shard, (s + 1) * shard)
            inside = slice(piece * shard, (piece + 1) * shard)
            cosine = turn_cos[at_rows, :]
            sine = -turn_sin[at_rows, :]
            grads = []
            for index_part in range(3):
                for pair in range(local // LANES):
                    if index_part == 0:
                        halves = [grad_q[2 * pair + e, inside, :] for e in range(2)]
                    else:
                        halves = [
                            grad_keys[2 * (2 * pair + e) + index_part - 1, at_rows, 0:HS]
                            for e in range(2)
                        ]
                    part = jnp.concatenate(halves, axis=1)
                    if index_part < 2:
                        part = turned(part, cosine, sine)
                    grads.append(part.astype(low))
            projected = jnp.concatenate(grads, axis=1)
            grad_proj[at_rows, 0 : 3 * local] = projected
            grad_one = dot(projected, wq[...], 1, 1)
            unit, _ = unit_rows(x_all[at_rows, :].astype(full))
            vectors[0:1, 0:width] += jnp.sum(grad_one * unit, axis=0, keepdims=True)
            vectors[1:2, 0:width] += jnp.sum(grad_one, axis=0, keepdims=True)
            u_all[at_rows, :] += grad_one * gain_one
            grad_chain_step(step_done)
            step_done += 1
        if slots:
            for _ in slots.pop(0)():
                pass

    while slots:
        slots.pop(0)()

    def vec_put(slots_ref, base, mine, peer, device):
        return remote(
            vectors,
            slots_ref.at[mine],
            vec_send.at[base + peer],
            vec_recv.at[base + mine],
            **device,
        )

    def vec_round(slots_ref, base, mine, size, device_of):
        others = [lax.rem(mine + step, size) for step in range(1, size)]
        for peer in others:
            vec_put(slots_ref, base, mine, peer, device_of(peer)).start()
        slots_ref[mine] = vectors[...]

        def finish():
            for peer in others:
                vec_put(slots_ref, base, mine, peer, device_of(peer)).wait_send()
                remote(
                    slots_ref.at[peer], slots_ref.at[peer],
                    vec_send.at[base + peer], vec_recv.at[base + peer], tensor=t,
                ).wait_recv()
            vectors[...] = total([slots_ref[index] for index in range(size)])

        return finish

    finish_vec = vec_round(vec_tensor, 0, t, ring, lambda peer: dict(tensor=peer))

    up_sum.stage(4)
    down_sum.stage(5)
    up_sum.stage(5)
    down_sum.stage(6)
    copy_down = pltpu.make_async_copy(done0, grad_down_out, out_sem.at[0])
    copy_down.start()
    part_mix, done_mix = part1, done1
    for block in range(width // BLOCK):
        part_mix[block_rows(block), 0 : 3 * local] = dot(
            normed_one[:, block_rows(block)], grad_proj[:, 0 : 3 * local], 0, 0
        ).astype(low)
    up_sum.stage(6)
    copy_up = pltpu.make_async_copy(done1, grad_up_out, out_sem.at[1])
    copy_up.start()
    copy_up.wait()
    copy_down.wait()
    for block in range(width // local):
        cols = slice(block * local, (block + 1) * local)
        part_mix[cols, 3 * local :] = dot(
            heads_side_by_side(context, slice(None)), g_all[:, cols], 0, 0
        ).astype(low)
    mix_sum = DataSum(
        spots, (part_mix, done_mix, half1, a11, b11, a21, b21), data_send.at[2], data_recv.at[2]
    )
    mix_sum.stage(0)
    finish_vec()
    finish_vec = vec_round(
        vec_core, ring, core, 2, lambda peer: dict(dp=dp_of(peer, x_at, y_at))
    )
    grad_chain_step(ring)
    mix_sum.stage(1)
    finish_vec()
    finish_vec = vec_round(
        vec_x, ring + 2, x_at, nx, lambda peer: dict(dp=dp_of(core, peer, y_at))
    )
    mix_sum.stage(2)
    finish_vec()
    finish_vec = vec_round(
        vec_y, ring + 2 + nx, y_at, 2, lambda peer: dict(dp=dp_of(core, x_at, peer))
    )
    for j in range(ring + 1, 2 * ring - 2):
        grad_chain_step(j)
    mix_sum.stage(3)
    finish_vec()
    rows_all = group * ranks
    rms_active = jnp.sqrt(jnp.sum(vectors[4:5, :], axis=1, keepdims=True) / (rows_all * FF))
    rms_context = jnp.sqrt(jnp.sum(vectors[5:6, :], axis=1, keepdims=True) / (rows_all * width))
    vectors_out[0:4, :] = vectors[0:4, :]
    vectors_out[4:5, :] = jnp.broadcast_to(rms_context, (1, vectors.shape[1]))
    vectors_out[5:6, :] = jnp.broadcast_to(rms_active, (1, vectors.shape[1]))
    vectors_out[6:8, :] = jnp.zeros_like(vectors_out[6:8, :])
    mix_sum.stage(4)
    weighted = grad_own()
    unit, scale = unit_rows(tokens[...].astype(full))
    grad_rows = scale * (
        weighted
        - jnp.mean(weighted, axis=-1, keepdims=True)
        - unit * jnp.mean(weighted * unit, axis=-1, keepdims=True)
    )
    input_grad[...] = (cotangent[...].astype(full) + grad_rows).astype(low)
    mix_sum.stage(5)
    mix_sum.stage(6)
    copy_mix = pltpu.make_async_copy(done_mix, grad_mix_out, out_sem.at[2])
    copy_mix.start()
    gather_drain(0)
    gather_drain(1)
    branch_drain()
    grad_drain()
    copy_mix.wait()


def per_device(
    ring, ranks,
    tokens, segments, w_qkv, w_out, w_up, w_down,
    gain_one, shift_one, gain_two, shift_two, cotangent,
):
    shard, width = tokens.shape
    group = segments.shape[1]
    local = w_qkv.shape[2]
    heads = local // HS
    hidden_local = w_up.shape[1]
    nx = ranks // 4
    half_rot = ROT // 2
    lane = jnp.arange(width) % HS
    frequency = rotary_base ** (-(2.0 * (lane % half_rot).astype(jnp.float32)) / ROT)
    frequency = jnp.where(lane < ROT, frequency, 0.0)
    sign = jnp.where(lane < half_rot, -1.0, 1.0)
    zero = jnp.zeros((width,), jnp.float32)
    norms = jnp.stack([gain_one, shift_one, gain_two, shift_two, frequency, sign, zero, zero])
    vmem = pl.BlockSpec(memory_space=pltpu.VMEM)
    anywhere = pl.BlockSpec(memory_space=pl.ANY)
    wide = max(width, hidden_local)
    scratch = lambda *shape: pltpu.VMEM(shape, low)
    wider = lambda *shape: pltpu.VMEM(shape, full)
    sems = lambda *shape: pltpu.SemaphoreType.DMA(shape)

    def sum_buffers(rows, columns):
        return [
            scratch(rows, columns),
            scratch(rows, columns),
            scratch(rows // 2, columns),
            scratch(nx, rows // (4 * nx), columns),
            scratch(2, rows // 8, columns),
            scratch(2, rows // (8 * nx), columns),
            scratch(nx, rows // (8 * nx), columns),
        ]

    data_sems = 12 + 4 * nx
    outs = pl.pallas_call(
        partial(layer_kernel, ring, ranks),
        name="layer",
        out_shape=[
            jax.ShapeDtypeStruct((shard, width), low),
            jax.ShapeDtypeStruct((shard, width), low),
            jax.ShapeDtypeStruct((hidden_local, width), low),
            jax.ShapeDtypeStruct((width, hidden_local), low),
            jax.ShapeDtypeStruct((width, 4 * local), low),
            jax.ShapeDtypeStruct((8, wide), full),
        ],
        in_specs=[vmem] * 5 + [anywhere] * 4,
        out_specs=[vmem, vmem, anywhere, anywhere, anywhere, vmem],
        scratch_shapes=[
            scratch(width, 3 * local), scratch(local, width),
            scratch(width, hidden_local), scratch(hidden_local, width),
            sems(4), sems(3),
            scratch(group, width), scratch(group, width),
            scratch(group, width), scratch(group, width),
            scratch(group, hidden_local),
            wider(hidden_local // LANES, group, LANES),
            wider(group, width),
            wider(hidden_local, width), wider(width, hidden_local),
            scratch(heads, group, HS), scratch(heads, group, HS), scratch(heads, group, HS),
            scratch(heads, group, HS), scratch(heads, group, HS),
            wider(heads, 1, group),
            wider(heads, BLOCK, HS),
            wider(group, LANES), wider(group, LANES),
            sems(2, 2, ring), sems(2, ring),
            scratch(ring + 1, shard, width), sems(ring), sems(ring + 1),
            scratch(ring + 1, shard, width), sems(ring), sems(ring + 1),
            *sum_buffers(hidden_local, width),
            *sum_buffers(width, hidden_local)[1:],
            sems(3, data_sems), sems(3, data_sems),
            wider(8, wide), wider(ring, 8, wide), wider(2, 8, wide),
            wider(nx, 8, wide), wider(2, 8, wide),
            sems(ring + 4 + nx), sems(ring + 4 + nx),
        ],
        compiler_params=pltpu.CompilerParams(
            collective_id=0, has_side_effects=True, vmem_limit_bytes=67043328
        ),
    )(
        tokens, cotangent, segments.reshape(group, 1), segments, norms,
        w_qkv.reshape(width, 3 * local), w_out, w_up, w_down,
    )
    output_rows, input_grad, grad_down, grad_up, grad_mix, vectors = outs
    grad_qkv = grad_mix[:, : 3 * local].astype(jnp.float32).reshape(width, 3, local)
    grad_out = (
        grad_mix[:, 3 * local :]
        .reshape(width // local, local, local)
        .transpose(1, 0, 2)
        .reshape(local, width)
        .astype(jnp.float32)
    )
    return (
        output_rows,
        input_grad,
        grad_qkv,
        grad_out,
        grad_up.astype(jnp.float32),
        grad_down.astype(jnp.float32),
        vectors[0, :width],
        vectors[1, :width],
        vectors[2, :width],
        vectors[3, :width],
        vectors[4, 0],
        vectors[5, 0],
    )


def solution(mesh):
    everyone = P(("dp", "tensor"), None)
    return jax.shard_map(
        partial(per_device, mesh.shape["tensor"], mesh.shape["dp"]),
        mesh=mesh,
        in_specs=(
            everyone,
            P("dp", None),
            P(None, None, "tensor"),
            P("tensor", None),
            P(None, "tensor"),
            P("tensor", None),
            P(),
            P(),
            P(),
            P(),
            everyone,
        ),
        out_specs=(
            everyone,
            everyone,
            P(None, None, "tensor"),
            P("tensor", None),
            P(None, "tensor"),
            P("tensor", None),
            P(),
            P(),
            P(),
            P(),
            P(),
            P(),
        ),
        check_vma=False,
    )
```

```python
from functools import partial, reduce

import jax
import jax.numpy as jnp
import numpy as np
from jax import lax
from jax.experimental import pallas as pl
from jax.experimental.pallas import tpu as pltpu
from jax.sharding import PartitionSpec as P

HS = 64
ROT = 16
FF = 4096
BLOCK = 256
LONGEST = 512
LANES = 128

epsilon = 1e-05
rotary_base = 10000.0
masked_score = -1000000000.0
low = jnp.bfloat16
full = jnp.float32
MESH = pl.DeviceIdType.MESH


def dot(a, b, over_a, over_b):
    return lax.dot_general(
        a, b, (((over_a,), (over_b,)), ((), ())), preferred_element_type=jnp.float32
    )


def total(parts):
    return reduce(jnp.add, parts)


def unit_rows(values):
    average = jnp.mean(values, axis=-1, keepdims=True)
    centred = values - average
    variance = jnp.mean(centred * centred, axis=-1, keepdims=True)
    scale = lax.rsqrt(variance + epsilon)
    return centred * scale, scale


def block_rows(index):
    return slice(index * BLOCK, (index + 1) * BLOCK)


def key_blocks(index):
    reach = (LONGEST + BLOCK - 2) // BLOCK
    return range(max(0, index - reach), index + 1)


def scores_turned(query, keys, seg_col, segment_row, head, at, key_at):
    scores = dot(keys[head, block_rows(key_at), :], query, 1, 1) * HS ** (-0.5)
    allowed = seg_col[block_rows(key_at), :] == segment_row[:, block_rows(at)]
    if at == key_at:
        key_index = lax.broadcasted_iota(jnp.int32, (BLOCK, BLOCK), 0)
        query_index = lax.broadcasted_iota(jnp.int32, (BLOCK, BLOCK), 1)
        allowed = allowed & (key_index <= query_index)
    return jnp.where(allowed, scores, masked_score)


def remote(source, target, send, receive, **device):
    return pltpu.make_async_remote_copy(
        source, target, send, receive, device_id=device, device_id_type=MESH
    )


class DataSum:
    def __init__(self, spots, bufs, send, receive):
        self.part, self.done, self.half, self.a1, self.b1, self.a2, self.b2 = bufs
        self.core, self.x, self.y, self.nx = spots
        self.send, self.receive = send, receive
        rows = self.part.shape[0]
        self.rows = rows
        self.open = []

    def dp(self, core=None, x=None, y=None):
        core = self.core if core is None else core
        x = self.x if x is None else x
        y = self.y if y is None else y
        return (y * self.nx + x) * 2 + core

    def rows_at(self, start, size):
        return pl.ds(pl.multiple_of(start, size), size)

    def put(self, source, target, base, mine, peer, device):
        copy = remote(
            source, target, self.send.at[base + peer], self.receive.at[base + mine], dp=device
        )
        copy.start()
        self.open.append(copy)

    def take(self, target, base, peer):
        remote(
            target, target, self.send.at[base + peer], self.receive.at[base + peer],
            dp=self.dp(),
        ).wait_recv()

    def drain(self):
        for copy in self.open:
            copy.wait_send()
        self.open = []

    def seat(self, sender, receiver):
        return lax.rem(sender - receiver - 1 + 2 * self.nx, self.nx)

    def x_peers(self):
        return [lax.rem(self.x + step, self.nx) for step in range(1, self.nx)]

    def bases(self):
        nx = self.nx
        names = {}
        at = 0
        for name, size in (
            ("c", 2), ("a1", nx), ("b1", 2), ("a2", 2), ("b2", nx),
            ("a3", 2), ("b3", nx), ("a4", nx), ("b4", 2), ("d", 2),
        ):
            names[name] = at
            at += size
        names["all"] = at
        return names

    def stage(self, number):
        rows, nx, core, x, y = self.rows, self.nx, self.core, self.x, self.y
        base = self.bases()
        half, quarter, eighth = rows // 2, rows // 4, rows // 8
        a_size, b_size, tail = quarter // nx, eighth, eighth // nx
        other, across = 1 - core, 1 - y
        start = core * half
        if number == 0:
            self.put(
                self.part.at[self.rows_at(other * half, half), :], self.half,
                base["c"], core, other, self.dp(core=other),
            )
        if number == 1:
            self.take(self.half, base["c"], other)
            add_rows(
                self.half, 0, [(self.part, start), (self.half, 0)], half
            )
            self.drain()
            for peer in self.x_peers():
                self.put(
                    self.half.at[self.rows_at(peer * a_size, a_size), :], self.a1.at[self.seat(x, peer)],
                    base["a1"], x, peer, self.dp(x=peer),
                )
            self.put(
                self.half.at[self.rows_at(quarter + across * b_size, b_size), :], self.b1.at[0],
                base["b1"], y, across, self.dp(y=across),
            )
        if number == 2:
            for peer in self.x_peers():
                self.take(self.a1.at[self.seat(peer, x)], base["a1"], peer)
            add_rows(
                self.half, x * a_size,
                [(self.half, x * a_size)] + [(self.a1.at[self.seat(peer, x)], 0) for peer in self.x_peers()],
                a_size,
            )
            self.take(self.b1.at[0], base["b1"], across)
            add_rows(
                self.half, quarter + y * b_size,
                [(self.half, quarter + y * b_size), (self.b1.at[0], 0)],
                b_size,
            )
            self.drain()
            self.put(
                self.half.at[self.rows_at(x * a_size + across * tail, tail), :], self.a2.at[0],
                base["a2"], y, across, self.dp(y=across),
            )
            for peer in self.x_peers():
                self.put(
                    self.half.at[self.rows_at(quarter + y * b_size + peer * tail, tail), :],
                    self.b2.at[self.seat(x, peer)], base["b2"], x, peer, self.dp(x=peer),
                )
        if number == 3:
            a_own = x * a_size + y * tail
            b_own = quarter + y * b_size + x * tail
            self.take(self.a2.at[0], base["a2"], across)
            add_rows(
                self.done, start + a_own, [(self.half, a_own), (self.a2.at[0], 0)], tail
            )
            for peer in self.x_peers():
                self.take(self.b2.at[self.seat(peer, x)], base["b2"], peer)
            add_rows(
                self.done, start + b_own,
                [(self.half, b_own)] + [(self.b2.at[self.seat(peer, x)], 0) for peer in self.x_peers()],
                tail,
            )
            self.drain()
            piece = self.done.at[self.rows_at(start + a_own, tail), :]
            self.put(piece, piece, base["a3"], y, across, self.dp(y=across))
            piece = self.done.at[self.rows_at(start + b_own, tail), :]
            for peer in self.x_peers():
                self.put(piece, piece, base["b3"], x, peer, self.dp(x=peer))
        if number == 4:
            self.take(
                self.done.at[self.rows_at(start + x * a_size + across * tail, tail), :],
                base["a3"], across,
            )
            for peer in self.x_peers():
                self.take(
                    self.done.at[
                        self.rows_at(start + quarter + y * b_size + peer * tail, tail), :
                    ],
                    base["b3"], peer,
                )
            self.drain()
            piece = self.done.at[self.rows_at(start + x * a_size, a_size), :]
            for peer in self.x_peers():
                self.put(piece, piece, base["a4"], x, peer, self.dp(x=peer))
            piece = self.done.at[self.rows_at(start + quarter + y * b_size, b_size), :]
            self.put(piece, piece, base["b4"], y, across, self.dp(y=across))
        if number == 5:
            for peer in self.x_peers():
                self.take(
                    self.done.at[self.rows_at(start + peer * a_size, a_size), :],
                    base["a4"], peer,
                )
            self.take(
                self.done.at[self.rows_at(start + quarter + across * b_size, b_size), :],
                base["b4"], across,
            )
            self.drain()
            piece = self.done.at[self.rows_at(start, half), :]
            self.put(piece, piece, base["d"], core, other, self.dp(core=other))
        if number == 6:
            self.take(self.done.at[self.rows_at(other * half, half), :], base["d"], other)
            self.drain()


def add_rows(target, target_start, sources, size):
    step = min(size, 64)

    def one(index, carry):
        offset = index * step

        def rows(start):
            return pl.ds(pl.multiple_of(start + offset, min(step, 16)), step)

        summed = total([ref[rows(start), :].astype(full) for ref, start in sources])
        target[rows(target_start), :] = summed.astype(target.dtype)
        return carry

    lax.fori_loop(0, size // step, one, 0)


def layer_kernel(
    ring,
    ranks,
    tokens, cotangent, seg_row, gains_one, shifts_one, gains_two, shifts_two, table,
    w_qkv, w_out, w_up, w_down,
    output_rows, input_grad, grad_down_out, grad_up_out, grad_qkv_out, grad_out_out, vectors_out,
    wq, wo, wu, wd, load_sem, out_sem,
    seg_col, x_all, g_all, normed_two, active, slope, u_all,
    acc_down, acc_up, queries, keys, values, grad_context, context, logs,
    grad_q, turn_cos, turn_sin,
    gather_send, gather_recv,
    branch_buf, branch_send, branch_recv, grad_buf, grad_send, grad_recv,
    part0, done0, half0, a10, b10, a20, b20,
    done1, half1, a11, b11, a21, b21,
    done2, half2, a12, b12, a22, b22,
    data_send, data_recv,
    vectors, vec_tensor, vec_core, vec_x, vec_y, vec_send, vec_recv,
):
    group = x_all.shape[0]
    width = x_all.shape[1]
    shard = group // ring
    heads = queries.shape[0]
    local = heads * HS
    blocks = group // BLOCK
    hidden_local = wu.shape[1]
    hidden_part = min(hidden_local, BLOCK)
    nx = ranks // 4
    part1 = wu
    grad_proj = normed_two
    t = lax.axis_index("tensor")
    dp = lax.axis_index("dp")
    core = lax.rem(dp, 2)
    x_at = lax.rem(dp // 2, nx)
    y_at = dp // (2 * nx)
    spots = (core, x_at, y_at, nx)

    def rows(s):
        return pl.ds(pl.multiple_of(s * shard, shard), shard)

    def dp_of(c, x, y):
        return (y * nx + x) * 2 + c

    pairs = [(tokens, x_all.at[rows(t), :]), (cotangent, g_all.at[rows(t), :])]
    pairs += [
        (w_qkv.at[part], wq.at[:, part * local : (part + 1) * local]) for part in range(3)
    ]
    pairs += [(w_up, wu), (w_out, wo), (w_down, wd)]
    loads = [
        pltpu.make_async_copy(source, target, load_sem.at[index])
        for index, (source, target) in enumerate(pairs)
    ]
    for copy in loads:
        copy.start()

    barrier = pltpu.get_barrier_semaphore()
    peers = [dict(tensor=lax.rem(t + step, ring)) for step in range(1, ring)]
    peers.append(dict(dp=dp_of(1 - core, x_at, y_at)))
    peers.append(dict(dp=dp_of(core, x_at, 1 - y_at)))
    for step in range(1, nx):
        peers.append(dict(dp=dp_of(core, lax.rem(x_at + step, nx), y_at)))
    for peer in peers:
        pl.semaphore_signal(barrier, inc=1, device_id=peer, device_id_type=MESH)
    pl.semaphore_wait(barrier, len(peers))

    def relay(which, source, s, side):
        target = (x_all, g_all)[which].at[rows(s), :]
        return remote(
            source,
            target,
            gather_send.at[which, side, s],
            gather_recv.at[which, s],
            tensor=t + 1 if side == 0 else t - 1,
        )

    def arrive(which, s):
        target = (x_all, g_all)[which].at[rows(s), :]
        remote(
            target, target, gather_send.at[which, 0, s], gather_recv.at[which, s], tensor=t
        ).wait_recv()

    def gather_step(which, k):
        array = (x_all, g_all)[which]

        @pl.when((k > 0) & (t - k >= 0))
        def _():
            s = t - k
            arrive(which, s)

            @pl.when(t < ring - 1)
            def _():
                relay(which, array.at[rows(s), :], s, 0).start()

        @pl.when((k > 0) & (t + k < ring))
        def _():
            s = t + k
            arrive(which, s)

            @pl.when(t > 0)
            def _():
                relay(which, array.at[rows(s), :], s, 1).start()

    def gather_own(which, side):
        relay(which, (tokens, cotangent)[which], t, side).start()

    def gather_drain(which):
        array = (x_all, g_all)[which]

        def one(s, carry):
            @pl.when((s <= t) & (t < ring - 1))
            def _():
                relay(which, array.at[rows(s), :], s, 0).wait_send()

            @pl.when((s >= t) & (t > 0))
            def _():
                relay(which, array.at[rows(s), :], s, 1).wait_send()

            return carry

        lax.fori_loop(0, ring, one, 0)

    @pl.when(t < ring - 1)
    def _():
        gather_own(0, 0)

    @pl.when(t > 0)
    def _():
        gather_own(0, 1)

    segment_row = seg_row[...].astype(full)
    seg_col[...] = jnp.broadcast_to(segment_row, (LANES, group)).T[:, 0:1]
    vectors[...] = jnp.zeros_like(vectors)
    acc_down[...] = jnp.zeros_like(acc_down)
    acc_up[...] = jnp.zeros_like(acc_up)
    gain_one, shift_one = gains_one[...], shifts_one[...]
    gain_two, shift_two = gains_two[...], shifts_two[...]
    for copy in loads:
        copy.wait()

    lane = lax.broadcasted_iota(jnp.int32, (shard, LANES), 1) % HS

    def turned(part, cosine, sine):
        moved = jnp.where(
            lane < ROT // 2, pltpu.roll(part, LANES - ROT // 2, 1), pltpu.roll(part, ROT // 2, 1)
        )
        return part * cosine + moved * sine

    def forward_rows(s):
        at = rows(s)
        unit, _ = unit_rows(x_all[at, :].astype(full))
        one = (unit * gain_one + shift_one).astype(low)
        two = (unit * gain_two + shift_two).astype(low)
        normed_two[at, :] = two
        own_segments = seg_col[at, :]
        before = jnp.sum((segment_row < own_segments).astype(jnp.int32), axis=1, keepdims=True)
        index = lax.broadcasted_iota(jnp.int32, (shard, 1), 0) + s * shard
        position = (index - before).astype(full)
        angle = position * table[0:1, :]
        cosine = jnp.cos(angle)
        sine = jnp.sin(angle) * table[1:2, :]
        turn_cos[at, :] = cosine
        turn_sin[at, :] = sine
        projected = dot(one, wq[...], 1, 0)
        for index_part, ref in enumerate((queries, keys, values)):
            for pair in range(local // LANES):
                lo = index_part * local + pair * LANES
                part = projected[:, lo : lo + LANES]
                if index_part < 2:
                    part = turned(part, cosine, sine)
                part = part.astype(low)
                for side in range(LANES // HS):
                    ref[pair * (LANES // HS) + side, at, :] = part[:, side * HS : (side + 1) * HS]
        for lo in range(0, hidden_local, hidden_part):
            span = slice(lo, lo + hidden_part)
            hidden = dot(two, wu[:, span], 1, 0)
            inner = 0.5 * (1.0 + lax.erf(hidden * 0.7071067811865476))
            activated = hidden * inner
            steep = inner + hidden * jnp.exp(-0.5 * hidden * hidden) * 0.3989422804014327
            active[at, span] = activated.astype(low)
            for chunk in range(hidden_part // LANES):
                slope[lo // LANES + chunk, at, :] = steep[:, chunk * LANES : (chunk + 1) * LANES]
            vectors[4:5, span] += jnp.sum(activated * activated, axis=0, keepdims=True)

    def both_sides(k, body):
        def one(side, carry):
            s = jnp.where(side == 0, t - k, t + k)

            @pl.when((s >= 0) & (s < ring) & ((k > 0) | (side == 0)))
            def _():
                body(s)

            return carry

        lax.fori_loop(0, 2, one, 0)

    def forward_step(k, carry):
        gather_step(0, k)

        @pl.when((k == t) & (t < ring - 1))
        def _():
            gather_own(1, 0)

        @pl.when((k == ring - 1 - t) & (t > 0))
        def _():
            gather_own(1, 1)

        both_sides(k, forward_rows)
        return carry

    lax.fori_loop(0, ring, forward_step, 0)

    for at in range(blocks):

        def forward_head(head, carry, at=at):
            query = queries[head, block_rows(at), :]
            spans = key_blocks(at)
            scores = [
                scores_turned(query, keys, seg_col, segment_row, head, at, span) for span in spans
            ]
            most = reduce(jnp.maximum, [jnp.max(s, axis=0, keepdims=True) for s in scores])
            raised = [jnp.exp(s - most) for s in scores]
            summed = total([jnp.sum(e, axis=0, keepdims=True) for e in raised])
            share = 1.0 / summed
            logs[head, :, block_rows(at)] = most + jnp.log(summed)
            mixed = total(
                [
                    dot((e * share).astype(low), values[head, block_rows(span), :], 0, 0)
                    for e, span in zip(raised, spans)
                ]
            )
            context[head, block_rows(at), :] = mixed.astype(low)
            vectors[5:6, 0:HS] += jnp.sum(mixed * mixed, axis=0, keepdims=True)
            return carry

        lax.fori_loop(0, heads, forward_head, 0)

    def heads_side_by_side(ref, at):
        return jnp.concatenate([ref[head, at, :] for head in range(heads)], axis=1)

    def branch_rows(s):
        at = rows(s)
        return dot(heads_side_by_side(context, at), wo[...], 1, 0) + dot(
            active[at, :], wd[...], 1, 0
        )

    def chain(buffer, send, receive, make):
        def hop(s, side):
            if side == 0:
                slot = s
            else:
                slot = jnp.where(s == t - 1, ring, s)
            return remote(
                buffer.at[s],
                buffer.at[slot],
                send.at[s],
                receive.at[slot],
                tensor=t + 1 if side == 0 else t - 1,
            )

        def landed(slot):
            remote(buffer.at[slot], buffer.at[slot], send.at[0], receive.at[slot], tensor=t).wait_recv()

        def pass_on(s, side):
            has = t > 0 if side == 0 else t < ring - 1

            @pl.when(has)
            def _():
                landed(s)
                buffer[s] = (make(s) + buffer[s].astype(full)).astype(low)

            @pl.when(jnp.logical_not(has))
            def _():
                buffer[s] = make(s).astype(low)

            hop(s, side).start()

        def own():
            value = make(t)

            @pl.when(t > 0)
            def _():
                landed(t)

            @pl.when(t < ring - 1)
            def _():
                landed(ring)

            left = jnp.where(t > 0, buffer[t].astype(full), 0.0)
            right = jnp.where(t < ring - 1, buffer[ring].astype(full), 0.0)
            return value + left + right

        def drain():
            def one(s, carry):
                @pl.when(s > t)
                def _():
                    hop(s, 0).wait_send()

                @pl.when(s < t)
                def _():
                    hop(s, 1).wait_send()

                return carry

            lax.fori_loop(0, ring, one, 0)

        return pass_on, own, drain

    branch_pass, branch_own, branch_drain = chain(
        branch_buf, branch_send, branch_recv, branch_rows
    )

    def backward_rows(s):
        at = rows(s)
        grad = g_all[at, :]
        grad_two = None
        for lo in range(0, hidden_local, hidden_part):
            span = slice(lo, lo + hidden_part)
            steep = jnp.concatenate(
                [slope[lo // LANES + chunk, at, :] for chunk in range(hidden_part // LANES)],
                axis=1,
            )
            grad_hidden = (dot(grad, wd[span, :], 1, 1) * steep).astype(low)
            acc_down[span, :] += dot(active[at, span], grad, 0, 0)
            acc_up[:, span] += dot(normed_two[at, :], grad_hidden, 0, 0)
            more = dot(grad_hidden, wu[:, span], 1, 1)
            grad_two = more if grad_two is None else grad_two + more
        unit, _ = unit_rows(x_all[at, :].astype(full))
        vectors[2:3, 0:width] += jnp.sum(grad_two * unit, axis=0, keepdims=True)
        vectors[3:4, 0:width] += jnp.sum(grad_two, axis=0, keepdims=True)
        u_all[at, :] = grad_two * gain_two
        back = dot(grad, wo[...], 1, 1).astype(low)
        for head in range(heads):
            grad_context[head, at, :] = back[:, head * HS : (head + 1) * HS]

    def backward_step(k, carry):
        gather_step(1, k)

        @pl.when((t == 0) & (k < ring - 1))
        def _():
            branch_pass(ring - 1 - k, 0)

        @pl.when((t == ring - 1) & (k < ring - 1))
        def _():
            branch_pass(k, 1)

        both_sides(k, backward_rows)
        return carry

    lax.fori_loop(0, ring, backward_step, 0)

    def narrow(source, target):
        step = 64

        def one(index, carry):
            at = pl.ds(pl.multiple_of(index * step, step), step)
            target[at, :] = source[at, :].astype(low)
            return carry

        lax.fori_loop(0, source.shape[0] // step, one, 0)

    down_sum = DataSum(
        spots, (part0, done0, half0, a10, b10, a20, b20), data_send.at[0], data_recv.at[0]
    )
    up_sum = DataSum(
        spots, (part1, done1, half1, a11, b11, a21, b21), data_send.at[1], data_recv.at[1]
    )
    def branch_hop(p):
        s_up = ring - 2 - p + t

        @pl.when((t > 0) & (s_up > t) & (s_up < ring))
        def _():
            branch_pass(s_up, 0)

        s_down = p + 2 - ring + t

        @pl.when((t < ring - 1) & (s_down >= 0) & (s_down < t))
        def _():
            branch_pass(s_down, 1)

    narrow(acc_down, part0)
    down_sum.stage(0)
    narrow(acc_up, part1)
    up_sum.stage(0)
    branch_hop(0)
    branch_hops = list(range(1, ring - 2))
    down_sum.stage(1)
    up_sum.stage(1)

    def u_rows(s):
        return u_all[rows(s), :]

    grad_pass, grad_own, grad_drain = chain(grad_buf, grad_send, grad_recv, u_rows)

    def grad_chain_step(j):
        s_up = ring - 1 - j + 2 * t

        @pl.when((s_up > t) & (s_up < ring))
        def _():
            grad_pass(s_up, 0)

        s_down = 3 * (ring - 1) - 2 * t - j

        @pl.when((s_down >= 0) & (s_down < t))
        def _():
            grad_pass(s_down, 1)

    grad_keys = slope
    slots = [
        lambda: (down_sum.stage(2),),
        lambda: (up_sum.stage(2), down_sum.stage(3)),
        lambda: (up_sum.stage(3), down_sum.stage(4)),
    ]
    step_done = 0
    for at in reversed(range(blocks)):

        def backward_head(head, carry, at=at):
            query = queries[head, block_rows(at), :]
            grad = grad_context[head, block_rows(at), :]
            spans = key_blocks(at)
            log_total = logs[head, :, block_rows(at)]
            probs = [
                jnp.exp(
                    scores_turned(query, keys, seg_col, segment_row, head, at, span) - log_total
                )
                for span in spans
            ]
            grad_probs = [dot(values[head, block_rows(span), :], grad, 1, 1) for span in spans]
            inner = total(
                [jnp.sum(p * d, axis=0, keepdims=True) for p, d in zip(probs, grad_probs)]
            )
            grad_query = []
            for p, d, span in zip(probs, grad_probs, spans):
                grad_scores = (p * (d - inner)).astype(low)
                grad_value = dot(p.astype(low), grad, 1, 0)
                grad_key = dot(grad_scores, query, 1, 0) * HS ** (-0.5)
                grad_query.append(dot(grad_scores, keys[head, block_rows(span), :], 0, 0))
                if at == min(span + len(key_blocks(blocks)) - 1, blocks - 1):
                    grad_keys[2 * head, block_rows(span), 0:HS] = grad_key
                    grad_keys[2 * head + 1, block_rows(span), 0:HS] = grad_value
                else:
                    grad_keys[2 * head, block_rows(span), 0:HS] += grad_key
                    grad_keys[2 * head + 1, block_rows(span), 0:HS] += grad_value
            grad_q[head] = total(grad_query) * HS ** (-0.5)
            return carry

        lax.fori_loop(0, heads, backward_head, 0)

        per_block = BLOCK // shard
        for piece in reversed(range(per_block)):
            s = at * per_block + piece
            at_rows = slice(s * shard, (s + 1) * shard)
            inside = slice(piece * shard, (piece + 1) * shard)
            cosine = turn_cos[at_rows, :]
            sine = -turn_sin[at_rows, :]
            grads = []
            for index_part in range(3):
                for pair in range(local // LANES):
                    if index_part == 0:
                        halves = [grad_q[2 * pair + e, inside, :] for e in range(2)]
                    else:
                        halves = [
                            grad_keys[2 * (2 * pair + e) + index_part - 1, at_rows, 0:HS]
                            for e in range(2)
                        ]
                    part = jnp.concatenate(halves, axis=1)
                    if index_part < 2:
                        part = turned(part, cosine, sine)
                    grads.append(part.astype(low))
            projected = jnp.concatenate(grads, axis=1)
            grad_proj[at_rows, 0 : 3 * local] = projected
            grad_one = dot(projected, wq[...], 1, 1)
            unit, _ = unit_rows(x_all[at_rows, :].astype(full))
            vectors[0:1, 0:width] += jnp.sum(grad_one * unit, axis=0, keepdims=True)
            vectors[1:2, 0:width] += jnp.sum(grad_one, axis=0, keepdims=True)
            u_all[at_rows, :] += grad_one * gain_one
            grad_chain_step(step_done)
            step_done += 1
        if slots:
            slots.pop(0)()
        if branch_hops:
            branch_hop(branch_hops.pop(0))

    while slots:
        slots.pop(0)()
    for p in branch_hops:
        branch_hop(p)

    def vec_put(slots_ref, base, mine, peer, device):
        return remote(
            vectors,
            slots_ref.at[mine],
            vec_send.at[base + peer],
            vec_recv.at[base + mine],
            **device,
        )

    def vec_round(slots_ref, base, mine, size, device_of):
        others = [lax.rem(mine + step, size) for step in range(1, size)]
        for peer in others:
            vec_put(slots_ref, base, mine, peer, device_of(peer)).start()
        slots_ref[mine] = vectors[...]

        def finish():
            for peer in others:
                vec_put(slots_ref, base, mine, peer, device_of(peer)).wait_send()
                remote(
                    slots_ref.at[peer], slots_ref.at[peer],
                    vec_send.at[base + peer], vec_recv.at[base + peer], tensor=t,
                ).wait_recv()
            vectors[...] = total([slots_ref[index] for index in range(size)])

        return finish

    finish_vec = vec_round(vec_tensor, 0, t, ring, lambda peer: dict(tensor=peer))

    part_mix = part1
    gather_drain(1)
    def out_block(block, carry):
        cols = pl.ds(pl.multiple_of(block * local, local), local)
        part_mix[cols, 3 * local :] = dot(
            heads_side_by_side(context, slice(None)), g_all[:, cols], 0, 0
        ).astype(low)
        return carry

    lax.fori_loop(0, width // local, out_block, 0)

    def norm_again(s, carry):
        unit, _ = unit_rows(x_all[rows(s), :].astype(full))
        g_all[rows(s), :] = (unit * gain_one + shift_one).astype(low)
        return carry

    lax.fori_loop(0, ring, norm_again, 0)
    def mix_block(block, carry):
        span = pl.ds(pl.multiple_of(block * BLOCK, BLOCK), BLOCK)
        part_mix[span, 0 : 3 * local] = dot(
            g_all[:, span], grad_proj[:, 0 : 3 * local], 0, 0
        ).astype(low)
        return carry

    lax.fori_loop(0, width // BLOCK, mix_block, 0)
    mix_sum = DataSum(
        spots, (part_mix, done2, half2, a12, b12, a22, b22), data_send.at[2], data_recv.at[2]
    )
    mix_sum.stage(0)
    late = iter(range(ring, 3 * ring - 4))

    def late_step(count=1):
        for _, j in zip(range(count), late):
            grad_chain_step(j)

    up_sum.stage(4)
    late_step()
    mix_sum.stage(1)
    down_sum.stage(5)
    finish_vec()
    finish_vec = vec_round(
        vec_core, ring, core, 2, lambda peer: dict(dp=dp_of(peer, x_at, y_at))
    )
    late_step()
    up_sum.stage(5)
    mix_sum.stage(2)
    finish_vec()
    finish_vec = vec_round(
        vec_x, ring + 2, x_at, nx, lambda peer: dict(dp=dp_of(core, peer, y_at))
    )
    down_sum.stage(6)
    copies = [pltpu.make_async_copy(done0, grad_down_out, out_sem.at[0])]
    copies[-1].start()
    late_step()
    mix_sum.stage(3)
    up_sum.stage(6)
    copies.append(pltpu.make_async_copy(done1, grad_up_out, out_sem.at[1]))
    copies[-1].start()
    finish_vec()
    finish_vec = vec_round(
        vec_y, ring + 2 + nx, y_at, 2, lambda peer: dict(dp=dp_of(core, x_at, peer))
    )
    late_step(2 * ring)
    mix_sum.stage(4)
    branch_buf[t] = (x_all[rows(t), :].astype(full) + branch_own()).astype(low)
    copies.append(pltpu.make_async_copy(branch_buf.at[t], output_rows, out_sem.at[2]))
    copies[-1].start()
    own_cotangent = branch_buf.at[ring]
    own_load = pltpu.make_async_copy(cotangent, own_cotangent, load_sem.at[0])
    own_load.start()
    finish_vec()
    rows_all = group * ranks
    rms_active = jnp.sqrt(jnp.sum(vectors[4:5, :], axis=1, keepdims=True) / (rows_all * FF))
    rms_context = jnp.sqrt(jnp.sum(vectors[5:6, :], axis=1, keepdims=True) / (rows_all * width))
    vectors_out[0:4, :] = vectors[0:4, :]
    vectors_out[4:5, :] = jnp.broadcast_to(rms_context, (1, vectors.shape[1]))
    vectors_out[5:6, :] = jnp.broadcast_to(rms_active, (1, vectors.shape[1]))
    vectors_out[6:8, :] = jnp.zeros_like(vectors_out[6:8, :])
    weighted = grad_own()
    own_load.wait()
    unit, scale = unit_rows(x_all[rows(t), :].astype(full))
    grad_rows = scale * (
        weighted
        - jnp.mean(weighted, axis=-1, keepdims=True)
        - unit * jnp.mean(weighted * unit, axis=-1, keepdims=True)
    )
    grad_buf[t] = (own_cotangent[...].astype(full) + grad_rows).astype(low)
    copies.append(pltpu.make_async_copy(grad_buf.at[t], input_grad, out_sem.at[3]))
    copies[-1].start()
    mix_sum.stage(5)
    mix_sum.stage(6)
    for part in range(3):
        copies.append(
            pltpu.make_async_copy(
                done2.at[:, part * local : (part + 1) * local],
                grad_qkv_out.at[part],
                out_sem.at[4 + part],
            )
        )
        copies[-1].start()
    for block in range(width // local):
        cols = slice(block * local, (block + 1) * local)
        copies.append(
            pltpu.make_async_copy(
                done2.at[cols, 3 * local :], grad_out_out.at[:, cols], out_sem.at[7 + block]
            )
        )
        copies[-1].start()
    gather_drain(0)
    branch_drain()
    grad_drain()
    for copy in copies:
        copy.wait()


def widen_kernel(*refs):
    count = 6
    for source, target in zip(refs[:count], refs[count + 1 : 2 * count + 1]):
        target[...] = source[...].astype(target.dtype)
    vectors = refs[count]
    for index, target in enumerate(refs[2 * count + 1 :]):
        target[...] = vectors[index : index + 1, 0 : target.shape[1]]


def widen(arrays, vectors, width):
    steps = 8

    def spec(shape):
        block = list(shape)
        block[-2] //= steps
        lead = (0,) * (len(shape) - 2)
        return pl.BlockSpec(tuple(block), lambda i, lead=lead: (*lead, i, 0))

    kinds = [low, low, full, full, full, full]
    small = [(1, width)] * 4 + [(1, 1)] * 2
    whole = lambda shape: pl.BlockSpec(shape, lambda i: (0, 0))
    return pl.pallas_call(
        widen_kernel,
        name="widen",
        grid=(steps,),
        out_shape=[jax.ShapeDtypeStruct(a.shape, kind) for a, kind in zip(arrays, kinds)]
        + [jax.ShapeDtypeStruct(shape, full) for shape in small],
        in_specs=[spec(a.shape) for a in arrays] + [whole(vectors.shape)],
        out_specs=[spec(a.shape) for a in arrays] + [whole(shape) for shape in small],
    )(*arrays, vectors)


def per_device(
    ring, ranks,
    tokens, segments, w_qkv, w_out, w_up, w_down,
    gain_one, shift_one, gain_two, shift_two, cotangent,
):
    shard, width = tokens.shape
    group = segments.shape[1]
    local = w_qkv.shape[2]
    heads = local // HS
    hidden_local = w_up.shape[1]
    nx = ranks // 4
    half_rot = ROT // 2
    lane = np.arange(LANES) % HS
    frequency = rotary_base ** (-(2.0 * (lane % half_rot)) / ROT)
    frequency = np.where(lane < ROT, frequency, 0.0)
    sign = np.where(lane < half_rot, -1.0, 1.0)
    table = jnp.asarray(np.stack([frequency, sign] + [np.zeros(LANES)] * 6), jnp.float32)
    vmem = pl.BlockSpec(memory_space=pltpu.VMEM)
    anywhere = pl.BlockSpec(memory_space=pl.ANY)
    wide = max(width, hidden_local)
    scratch = lambda *shape: pltpu.VMEM(shape, low)
    wider = lambda *shape: pltpu.VMEM(shape, full)
    sems = lambda *shape: pltpu.SemaphoreType.DMA(shape)

    def sum_buffers(rows, columns):
        return [
            scratch(rows, columns),
            scratch(rows, columns),
            scratch(rows // 2, columns),
            scratch(nx - 1, rows // (4 * nx), columns),
            scratch(1, rows // 8, columns),
            scratch(1, rows // (8 * nx), columns),
            scratch(nx - 1, rows // (8 * nx), columns),
        ]

    data_sems = 12 + 4 * nx
    outs = pl.pallas_call(
        partial(layer_kernel, ring, ranks),
        name="layer",
        out_shape=[
            jax.ShapeDtypeStruct((shard, width), low),
            jax.ShapeDtypeStruct((shard, width), low),
            jax.ShapeDtypeStruct((hidden_local, width), low),
            jax.ShapeDtypeStruct((width, hidden_local), low),
            jax.ShapeDtypeStruct((3, width, local), low),
            jax.ShapeDtypeStruct((local, width), low),
            jax.ShapeDtypeStruct((8, wide), full),
        ],
        in_specs=[anywhere] * 2 + [vmem] * 6 + [anywhere] * 4,
        out_specs=[anywhere] * 6 + [vmem],
        scratch_shapes=[
            scratch(width, 3 * local), scratch(local, width),
            scratch(width, hidden_local), scratch(hidden_local, width),
            sems(8), sems(7 + width // local),
            wider(group, 1),
            scratch(group, width), scratch(group, width), scratch(group, width),
            scratch(group, hidden_local),
            wider(hidden_local // LANES, group, LANES),
            wider(group, width),
            wider(hidden_local, width), wider(width, hidden_local),
            scratch(heads, group, HS), scratch(heads, group, HS), scratch(heads, group, HS),
            scratch(heads, group, HS), scratch(heads, group, HS),
            wider(heads, 1, group),
            wider(heads, BLOCK, HS),
            wider(group, LANES), wider(group, LANES),
            sems(2, 2, ring), sems(2, ring),
            scratch(ring + 1, shard, width), sems(ring), sems(ring + 1),
            scratch(ring + 1, shard, width), sems(ring), sems(ring + 1),
            *sum_buffers(hidden_local, width),
            *sum_buffers(width, hidden_local)[1:],
            *sum_buffers(width, 4 * local)[1:],
            sems(3, data_sems), sems(3, data_sems),
            wider(8, wide), wider(ring, 8, wide), wider(2, 8, wide),
            wider(nx, 8, wide), wider(2, 8, wide),
            sems(ring + 4 + nx), sems(ring + 4 + nx),
        ],
        compiler_params=pltpu.CompilerParams(
            collective_id=0, has_side_effects=True, vmem_limit_bytes=67043328
        ),
    )(
        tokens, cotangent, segments,
        *(v.reshape(1, width) for v in (gain_one, shift_one, gain_two, shift_two)), table,
        w_qkv.transpose(1, 0, 2), w_out, w_up, w_down,
    )
    output_rows, input_grad, grad_down, grad_up, grad_qkv, grad_out, *small = widen(
        outs[:6], outs[6], width
    )
    return (
        output_rows,
        input_grad,
        grad_qkv.transpose(1, 0, 2),
        grad_out,
        grad_up,
        grad_down,
        *(v.reshape(width) for v in small[:4]),
        small[4].reshape(()),
        small[5].reshape(()),
    )


def solution(mesh):
    everyone = P(("dp", "tensor"), None)
    return jax.shard_map(
        partial(per_device, mesh.shape["tensor"], mesh.shape["dp"]),
        mesh=mesh,
        in_specs=(
            everyone,
            P("dp", None),
            P(None, None, "tensor"),
            P("tensor", None),
            P(None, "tensor"),
            P("tensor", None),
            P(),
            P(),
            P(),
            P(),
            everyone,
        ),
        out_specs=(
            everyone,
            everyone,
            P(None, None, "tensor"),
            P("tensor", None),
            P(None, "tensor"),
            P("tensor", None),
            P(),
            P(),
            P(),
            P(),
            P(),
            P(),
        ),
        check_vma=False,
    )
```

```python
from functools import partial, reduce

import jax
import jax.numpy as jnp
import numpy as np
from jax import lax
from jax.experimental import pallas as pl
from jax.experimental.pallas import tpu as pltpu
from jax.sharding import PartitionSpec as P

HS = 64
ROT = 16
FF = 4096
BLOCK = 256
LONGEST = 512
LANES = 128
PIECES = 1

epsilon = 1e-05
rotary_base = 10000.0
masked_score = -1000000000.0
low = jnp.bfloat16
full = jnp.float32
MESH = pl.DeviceIdType.MESH


def dot(a, b, over_a, over_b):
    return lax.dot_general(
        a, b, (((over_a,), (over_b,)), ((), ())), preferred_element_type=jnp.float32
    )


def total(parts):
    return reduce(jnp.add, parts)


def unit_rows(values):
    average = jnp.mean(values, axis=-1, keepdims=True)
    centred = values - average
    variance = jnp.mean(centred * centred, axis=-1, keepdims=True)
    scale = lax.rsqrt(variance + epsilon)
    return centred * scale, scale


def block_rows(index):
    return slice(index * BLOCK, (index + 1) * BLOCK)


def key_blocks(index):
    reach = (LONGEST + BLOCK - 2) // BLOCK
    return range(max(0, index - reach), index + 1)


def scores_turned(query, keys, seg_col, segment_row, head, at, key_at):
    scores = dot(keys[head, block_rows(key_at), :], query, 1, 1) * HS ** (-0.5)
    allowed = seg_col[block_rows(key_at), :] == segment_row[:, block_rows(at)]
    if at == key_at:
        key_index = lax.broadcasted_iota(jnp.int32, (BLOCK, BLOCK), 0)
        query_index = lax.broadcasted_iota(jnp.int32, (BLOCK, BLOCK), 1)
        allowed = allowed & (key_index <= query_index)
    return jnp.where(allowed, scores, masked_score)


def remote(source, target, send, receive, **device):
    return pltpu.make_async_remote_copy(
        source, target, send, receive, device_id=device, device_id_type=MESH
    )


class DataSum:
    def __init__(self, spots, bufs, send, receive):
        self.part, self.done, self.half, self.a1, self.b1, self.a2, self.b2 = bufs
        self.core, self.x, self.y, self.nx = spots
        self.send, self.receive = send, receive
        rows = self.part.shape[0]
        self.rows = rows
        self.open = []

    def dp(self, core=None, x=None, y=None):
        core = self.core if core is None else core
        x = self.x if x is None else x
        y = self.y if y is None else y
        return (y * self.nx + x) * 2 + core

    def rows_at(self, start, size):
        return pl.ds(pl.multiple_of(start, size), size)

    def put(self, source, target, base, mine, peer, device):
        copy = remote(
            source, target, self.send.at[base + peer], self.receive.at[base + mine], dp=device
        )
        copy.start()
        self.open.append(copy)

    def take(self, target, base, peer):
        remote(
            target, target, self.send.at[base + peer], self.receive.at[base + peer],
            dp=self.dp(),
        ).wait_recv()

    def drain(self):
        for copy in self.open:
            copy.wait_send()
        self.open = []

    def seat(self, sender, receiver):
        return lax.rem(sender - receiver - 1 + 2 * self.nx, self.nx)

    def x_peers(self):
        return [lax.rem(self.x + step, self.nx) for step in range(1, self.nx)]

    def bases(self):
        nx = self.nx
        names = {}
        at = 0
        for name, size in (
            ("c", 2), ("a1", nx), ("b1", 2), ("a2", 2), ("b2", nx),
            ("a3", 2), ("b3", nx), ("a4", nx), ("b4", 2), ("d", 2),
        ):
            names[name] = at
            at += size
        names["all"] = at
        return names

    def stage(self, number):
        rows, nx, core, x, y = self.rows, self.nx, self.core, self.x, self.y
        base = self.bases()
        half, quarter, eighth = rows // 2, rows // 4, rows // 8
        a_size, b_size, tail = quarter // nx, eighth, eighth // nx
        other, across = 1 - core, 1 - y
        start = core * half
        if number == 0:
            self.put(
                self.part.at[self.rows_at(other * half, half), :], self.half,
                base["c"], core, other, self.dp(core=other),
            )
        if number == 1:
            self.take(self.half, base["c"], other)
            add_rows(
                self.half, 0, [(self.part, start), (self.half, 0)], half
            )
            self.drain()
            for peer in self.x_peers():
                self.put(
                    self.half.at[self.rows_at(peer * a_size, a_size), :], self.a1.at[self.seat(x, peer)],
                    base["a1"], x, peer, self.dp(x=peer),
                )
            self.put(
                self.half.at[self.rows_at(quarter + across * b_size, b_size), :], self.b1.at[0],
                base["b1"], y, across, self.dp(y=across),
            )
        if number == 2:
            for peer in self.x_peers():
                self.take(self.a1.at[self.seat(peer, x)], base["a1"], peer)
            add_rows(
                self.half, x * a_size,
                [(self.half, x * a_size)] + [(self.a1.at[self.seat(peer, x)], 0) for peer in self.x_peers()],
                a_size,
            )
            self.take(self.b1.at[0], base["b1"], across)
            add_rows(
                self.half, quarter + y * b_size,
                [(self.half, quarter + y * b_size), (self.b1.at[0], 0)],
                b_size,
            )
            self.drain()
            self.put(
                self.half.at[self.rows_at(x * a_size + across * tail, tail), :], self.a2.at[0],
                base["a2"], y, across, self.dp(y=across),
            )
            for peer in self.x_peers():
                self.put(
                    self.half.at[self.rows_at(quarter + y * b_size + peer * tail, tail), :],
                    self.b2.at[self.seat(x, peer)], base["b2"], x, peer, self.dp(x=peer),
                )
        if number == 3:
            a_own = x * a_size + y * tail
            b_own = quarter + y * b_size + x * tail
            self.take(self.a2.at[0], base["a2"], across)
            add_rows(
                self.done, start + a_own, [(self.half, a_own), (self.a2.at[0], 0)], tail
            )
            for peer in self.x_peers():
                self.take(self.b2.at[self.seat(peer, x)], base["b2"], peer)
            add_rows(
                self.done, start + b_own,
                [(self.half, b_own)] + [(self.b2.at[self.seat(peer, x)], 0) for peer in self.x_peers()],
                tail,
            )
            self.drain()
            piece = self.done.at[self.rows_at(start + a_own, tail), :]
            self.put(piece, piece, base["a3"], y, across, self.dp(y=across))
            piece = self.done.at[self.rows_at(start + b_own, tail), :]
            for peer in self.x_peers():
                self.put(piece, piece, base["b3"], x, peer, self.dp(x=peer))
        if number == 4:
            self.take(
                self.done.at[self.rows_at(start + x * a_size + across * tail, tail), :],
                base["a3"], across,
            )
            for peer in self.x_peers():
                self.take(
                    self.done.at[
                        self.rows_at(start + quarter + y * b_size + peer * tail, tail), :
                    ],
                    base["b3"], peer,
                )
            self.drain()
            piece = self.done.at[self.rows_at(start + x * a_size, a_size), :]
            for peer in self.x_peers():
                self.put(piece, piece, base["a4"], x, peer, self.dp(x=peer))
            piece = self.done.at[self.rows_at(start + quarter + y * b_size, b_size), :]
            self.put(piece, piece, base["b4"], y, across, self.dp(y=across))
        if number == 5:
            for peer in self.x_peers():
                self.take(
                    self.done.at[self.rows_at(start + peer * a_size, a_size), :],
                    base["a4"], peer,
                )
            self.take(
                self.done.at[self.rows_at(start + quarter + across * b_size, b_size), :],
                base["b4"], across,
            )
            self.drain()
            piece = self.done.at[self.rows_at(start, half), :]
            self.put(piece, piece, base["d"], core, other, self.dp(core=other))
        if number == 6:
            self.take(self.done.at[self.rows_at(other * half, half), :], base["d"], other)
            self.drain()


def add_rows(target, target_start, sources, size):
    step = min(size, 64)

    def one(index, carry):
        offset = index * step

        def rows(start):
            return pl.ds(pl.multiple_of(start + offset, min(step, 16)), step)

        summed = total([ref[rows(start), :].astype(full) for ref, start in sources])
        target[rows(target_start), :] = summed.astype(target.dtype)
        return carry

    lax.fori_loop(0, size // step, one, 0)


def layer_kernel(
    ring,
    ranks,
    tokens, cotangent, seg_row, gains_one, shifts_one, gains_two, shifts_two, table,
    w_qkv, w_out, w_up, w_down,
    output_rows, input_grad, grad_down_out, grad_up_out, grad_qkv_out, grad_out_out, vectors_out,
    wq, wo, wu, wd, load_sem, out_sem,
    seg_col, x_all, g_all, normed_two, active, slope, u_all,
    acc_down, acc_up, queries, keys, values, grad_context, context, logs,
    grad_q, turn_cos, turn_sin,
    gather_send, gather_recv,
    branch_buf, branch_send, branch_recv, grad_buf, grad_send, grad_recv,
    part0, done0, half0, a10, b10, a20, b20,
    done1, half1, a11, b11, a21, b21,
    done2, half2, a12, b12, a22, b22,
    data_send, data_recv,
    vectors, vec_tensor, vec_core, vec_x, vec_y, vec_send, vec_recv,
):
    group = x_all.shape[0]
    width = x_all.shape[1]
    shard = group // ring
    heads = queries.shape[0]
    local = heads * HS
    blocks = group // BLOCK
    hidden_local = wu.shape[1]
    hidden_part = min(hidden_local, BLOCK)
    nx = ranks // 4
    part1 = wu
    grad_proj = normed_two
    t = lax.axis_index("tensor")
    dp = lax.axis_index("dp")
    core = lax.rem(dp, 2)
    x_at = lax.rem(dp // 2, nx)
    y_at = dp // (2 * nx)
    spots = (core, x_at, y_at, nx)

    def rows(s):
        return pl.ds(pl.multiple_of(s * shard, shard), shard)

    def dp_of(c, x, y):
        return (y * nx + x) * 2 + c

    pairs = [(tokens, x_all.at[rows(t), :]), (cotangent, g_all.at[rows(t), :])]
    pairs += [
        (w_qkv.at[part], wq.at[:, part * local : (part + 1) * local]) for part in range(3)
    ]
    pairs += [(w_up, wu), (w_out, wo), (w_down, wd)]
    loads = [
        pltpu.make_async_copy(source, target, load_sem.at[index])
        for index, (source, target) in enumerate(pairs)
    ]
    for copy in loads:
        copy.start()

    barrier = pltpu.get_barrier_semaphore()
    peers = [dict(tensor=lax.rem(t + step, ring)) for step in range(1, ring)]
    peers.append(dict(dp=dp_of(1 - core, x_at, y_at)))
    peers.append(dict(dp=dp_of(core, x_at, 1 - y_at)))
    for step in range(1, nx):
        peers.append(dict(dp=dp_of(core, lax.rem(x_at + step, nx), y_at)))
    for peer in peers:
        pl.semaphore_signal(barrier, inc=1, device_id=peer, device_id_type=MESH)
    pl.semaphore_wait(barrier, len(peers))

    def relay(which, source, s, side):
        target = (x_all, g_all)[which].at[rows(s), :]
        return remote(
            source,
            target,
            gather_send.at[which, side, s],
            gather_recv.at[which, s],
            tensor=t + 1 if side == 0 else t - 1,
        )

    def arrive(which, s):
        target = (x_all, g_all)[which].at[rows(s), :]
        remote(
            target, target, gather_send.at[which, 0, s], gather_recv.at[which, s], tensor=t
        ).wait_recv()

    def gather_step(which, k):
        array = (x_all, g_all)[which]

        @pl.when((k > 0) & (t - k >= 0))
        def _():
            s = t - k
            arrive(which, s)

            @pl.when(t < ring - 1)
            def _():
                relay(which, array.at[rows(s), :], s, 0).start()

        @pl.when((k > 0) & (t + k < ring))
        def _():
            s = t + k
            arrive(which, s)

            @pl.when(t > 0)
            def _():
                relay(which, array.at[rows(s), :], s, 1).start()

    def gather_own(which, side):
        relay(which, (tokens, cotangent)[which], t, side).start()

    def gather_drain(which):
        array = (x_all, g_all)[which]

        def one(s, carry):
            @pl.when((s <= t) & (t < ring - 1))
            def _():
                relay(which, array.at[rows(s), :], s, 0).wait_send()

            @pl.when((s >= t) & (t > 0))
            def _():
                relay(which, array.at[rows(s), :], s, 1).wait_send()

            return carry

        lax.fori_loop(0, ring, one, 0)

    @pl.when(t < ring - 1)
    def _():
        gather_own(0, 0)

    @pl.when(t > 0)
    def _():
        gather_own(0, 1)

    segment_row = seg_row[...].astype(full)
    seg_col[...] = jnp.broadcast_to(segment_row, (LANES, group)).T[:, 0:1]
    vectors[...] = jnp.zeros_like(vectors)
    acc_down[...] = jnp.zeros_like(acc_down)
    acc_up[...] = jnp.zeros_like(acc_up)
    gain_one, shift_one = gains_one[...], shifts_one[...]
    gain_two, shift_two = gains_two[...], shifts_two[...]
    for copy in loads:
        copy.wait()

    lane = lax.broadcasted_iota(jnp.int32, (shard, LANES), 1) % HS

    def turned(part, cosine, sine):
        moved = jnp.where(
            lane < ROT // 2, pltpu.roll(part, LANES - ROT // 2, 1), pltpu.roll(part, ROT // 2, 1)
        )
        return part * cosine + moved * sine

    def forward_rows(s):
        at = rows(s)
        unit, _ = unit_rows(x_all[at, :].astype(full))
        one = (unit * gain_one + shift_one).astype(low)
        two = (unit * gain_two + shift_two).astype(low)
        normed_two[at, :] = two
        own_segments = seg_col[at, :]
        before = jnp.sum((segment_row < own_segments).astype(jnp.int32), axis=1, keepdims=True)
        index = lax.broadcasted_iota(jnp.int32, (shard, 1), 0) + s * shard
        position = (index - before).astype(full)
        angle = position * table[0:1, :]
        cosine = jnp.cos(angle)
        sine = jnp.sin(angle) * table[1:2, :]
        turn_cos[at, :] = cosine
        turn_sin[at, :] = sine
        projected = dot(one, wq[...], 1, 0)
        for index_part, ref in enumerate((queries, keys, values)):
            for pair in range(local // LANES):
                lo = index_part * local + pair * LANES
                part = projected[:, lo : lo + LANES]
                if index_part < 2:
                    part = turned(part, cosine, sine)
                part = part.astype(low)
                for side in range(LANES // HS):
                    ref[pair * (LANES // HS) + side, at, :] = part[:, side * HS : (side + 1) * HS]
        for lo in range(0, hidden_local, hidden_part):
            span = slice(lo, lo + hidden_part)
            hidden = dot(two, wu[:, span], 1, 0)
            inner = 0.5 * (1.0 + lax.erf(hidden * 0.7071067811865476))
            activated = hidden * inner
            steep = inner + hidden * jnp.exp(-0.5 * hidden * hidden) * 0.3989422804014327
            active[at, span] = activated.astype(low)
            for chunk in range(hidden_part // LANES):
                slope[lo // LANES + chunk, at, :] = steep[:, chunk * LANES : (chunk + 1) * LANES]
            vectors[4:5, span] += jnp.sum(activated * activated, axis=0, keepdims=True)

    def both_sides(k, body):
        def one(side, carry):
            s = jnp.where(side == 0, t - k, t + k)

            @pl.when((s >= 0) & (s < ring) & ((k > 0) | (side == 0)))
            def _():
                body(s)

            return carry

        lax.fori_loop(0, 2, one, 0)

    def forward_step(k, carry):
        gather_step(0, k)

        @pl.when((k == t) & (t < ring - 1))
        def _():
            gather_own(1, 0)

        @pl.when((k == ring - 1 - t) & (t > 0))
        def _():
            gather_own(1, 1)

        both_sides(k, forward_rows)
        return carry

    lax.fori_loop(0, ring, forward_step, 0)

    for at in range(blocks):

        def forward_head(head, carry, at=at):
            query = queries[head, block_rows(at), :]
            spans = key_blocks(at)
            scores = [
                scores_turned(query, keys, seg_col, segment_row, head, at, span) for span in spans
            ]
            most = reduce(jnp.maximum, [jnp.max(s, axis=0, keepdims=True) for s in scores])
            raised = [jnp.exp(s - most) for s in scores]
            summed = total([jnp.sum(e, axis=0, keepdims=True) for e in raised])
            share = 1.0 / summed
            logs[head, :, block_rows(at)] = most + jnp.log(summed)
            mixed = total(
                [
                    dot((e * share).astype(low), values[head, block_rows(span), :], 0, 0)
                    for e, span in zip(raised, spans)
                ]
            )
            context[head, block_rows(at), :] = mixed.astype(low)
            vectors[5:6, 0:HS] += jnp.sum(mixed * mixed, axis=0, keepdims=True)
            return carry

        lax.fori_loop(0, heads, forward_head, 0)

    def heads_side_by_side(ref, at):
        return jnp.concatenate([ref[head, at, :] for head in range(heads)], axis=1)

    def branch_rows(s):
        at = rows(s)
        return dot(heads_side_by_side(context, at), wo[...], 1, 0) + dot(
            active[at, :], wd[...], 1, 0
        )

    def chain(buffer, send, receive, make):
        def hop(s, side):
            if side == 0:
                slot = s
            else:
                slot = jnp.where(s == t - 1, ring, s)
            return remote(
                buffer.at[s],
                buffer.at[slot],
                send.at[s],
                receive.at[slot],
                tensor=t + 1 if side == 0 else t - 1,
            )

        def landed(slot):
            remote(buffer.at[slot], buffer.at[slot], send.at[0], receive.at[slot], tensor=t).wait_recv()

        def pass_on(s, side):
            has = t > 0 if side == 0 else t < ring - 1

            @pl.when(has)
            def _():
                landed(s)
                buffer[s] = (make(s) + buffer[s].astype(full)).astype(low)

            @pl.when(jnp.logical_not(has))
            def _():
                buffer[s] = make(s).astype(low)

            hop(s, side).start()

        def own():
            value = make(t)

            @pl.when(t > 0)
            def _():
                landed(t)

            @pl.when(t < ring - 1)
            def _():
                landed(ring)

            left = jnp.where(t > 0, buffer[t].astype(full), 0.0)
            right = jnp.where(t < ring - 1, buffer[ring].astype(full), 0.0)
            return value + left + right

        def drain():
            def one(s, carry):
                @pl.when(s > t)
                def _():
                    hop(s, 0).wait_send()

                @pl.when(s < t)
                def _():
                    hop(s, 1).wait_send()

                return carry

            lax.fori_loop(0, ring, one, 0)

        return pass_on, own, drain

    branch_pass, branch_own, branch_drain = chain(
        branch_buf, branch_send, branch_recv, branch_rows
    )

    def backward_rows(s):
        at = rows(s)
        grad = g_all[at, :]
        grad_two = None
        for lo in range(0, hidden_local, hidden_part):
            span = slice(lo, lo + hidden_part)
            steep = jnp.concatenate(
                [slope[lo // LANES + chunk, at, :] for chunk in range(hidden_part // LANES)],
                axis=1,
            )
            grad_hidden = (dot(grad, wd[span, :], 1, 1) * steep).astype(low)
            acc_down[span, :] += dot(active[at, span], grad, 0, 0)
            acc_up[:, span] += dot(normed_two[at, :], grad_hidden, 0, 0)
            more = dot(grad_hidden, wu[:, span], 1, 1)
            grad_two = more if grad_two is None else grad_two + more
        unit, _ = unit_rows(x_all[at, :].astype(full))
        vectors[2:3, 0:width] += jnp.sum(grad_two * unit, axis=0, keepdims=True)
        vectors[3:4, 0:width] += jnp.sum(grad_two, axis=0, keepdims=True)
        u_all[at, :] = grad_two * gain_two
        back = dot(grad, wo[...], 1, 1).astype(low)
        for head in range(heads):
            grad_context[head, at, :] = back[:, head * HS : (head + 1) * HS]

    def backward_step(k, carry):
        gather_step(1, k)

        @pl.when((t == 0) & (k < ring - 1))
        def _():
            branch_pass(ring - 1 - k, 0)

        @pl.when((t == ring - 1) & (k < ring - 1))
        def _():
            branch_pass(k, 1)

        both_sides(k, backward_rows)
        return carry

    lax.fori_loop(0, ring, backward_step, 0)

    def narrow(source, target):
        step = 64

        def one(index, carry):
            at = pl.ds(pl.multiple_of(index * step, step), step)
            target[at, :] = source[at, :].astype(low)
            return carry

        lax.fori_loop(0, source.shape[0] // step, one, 0)

    down_sum = DataSum(
        spots, (part0, done0, half0, a10, b10, a20, b20), data_send.at[0], data_recv.at[0]
    )
    up_sum = DataSum(
        spots, (part1, done1, half1, a11, b11, a21, b21), data_send.at[1], data_recv.at[1]
    )
    def branch_hop(p):
        s_up = ring - 2 - p + t

        @pl.when((t > 0) & (s_up > t) & (s_up < ring))
        def _():
            branch_pass(s_up, 0)

        s_down = p + 2 - ring + t

        @pl.when((t < ring - 1) & (s_down >= 0) & (s_down < t))
        def _():
            branch_pass(s_down, 1)

    narrow(acc_down, part0)
    down_sum.stage(0)
    narrow(acc_up, part1)
    up_sum.stage(0)
    branch_hop(0)
    branch_hops = list(range(1, ring - 2))
    down_sum.stage(1)
    up_sum.stage(1)

    part_rows = shard // PIECES

    def u_hop(s, piece, side):
        at = pl.ds(pl.multiple_of(piece * part_rows, part_rows), part_rows)
        slot = s if side == 0 else jnp.where(s == t - 1, ring, s)
        return remote(
            grad_buf.at[s, at, :],
            grad_buf.at[slot, at, :],
            grad_send.at[s, piece],
            grad_recv.at[slot, piece],
            tensor=t + 1 if side == 0 else t - 1,
        )

    def u_landed(slot, piece):
        at = pl.ds(pl.multiple_of(piece * part_rows, part_rows), part_rows)
        ref = grad_buf.at[slot, at, :]
        remote(ref, ref, grad_send.at[0, piece], grad_recv.at[slot, piece], tensor=t).wait_recv()

    def each_piece(body):
        def one(piece, carry):
            body(piece)
            return carry

        lax.fori_loop(0, PIECES, one, 0)

    def u_start(s):
        for side, end in ((0, 0), (1, ring - 1)):
            if s == end:
                continue

            @pl.when(t == end)
            def _(side=side):
                grad_buf[s] = u_all[rows(s), :].astype(low)
                each_piece(lambda piece: u_hop(s, piece, side).start())

    def u_pass(s, piece, side):
        u_landed(s, piece)
        at = pl.ds(pl.multiple_of(piece * part_rows, part_rows), part_rows)
        source = pl.ds(pl.multiple_of(s * shard + piece * part_rows, part_rows), part_rows)
        grad_buf[s, at, :] = (u_all[source, :] + grad_buf[s, at, :].astype(full)).astype(low)
        u_hop(s, piece, side).start()

    def u_step(tick, carry):
        up = tick - 2 * t
        s_up = ring - 1 - up // PIECES

        @pl.when((t > 0) & (up >= 0) & (s_up > t))
        def _():
            u_pass(s_up, lax.rem(up, PIECES), 0)

        down = tick + 2 - 2 * (ring - 1 - t)
        s_down = ring - 1 - down // PIECES

        @pl.when((t < ring - 1) & (down >= 0) & (s_down >= 0) & (s_down < t))
        def _():
            u_pass(s_down, lax.rem(down, PIECES), 1)

        return carry

    def u_steps(first, last):
        lax.fori_loop(first, last, u_step, 0)

    def u_own():
        @pl.when(t > 0)
        def _():
            each_piece(lambda piece: u_landed(t, piece))

        @pl.when(t < ring - 1)
        def _():
            each_piece(lambda piece: u_landed(ring, piece))

        left = jnp.where(t > 0, grad_buf[t].astype(full), 0.0)
        right = jnp.where(t < ring - 1, grad_buf[ring].astype(full), 0.0)
        return u_all[rows(t), :] + left + right

    def u_drain():
        def one(s, carry):
            @pl.when(s > t)
            def _():
                each_piece(lambda piece: u_hop(s, piece, 0).wait_send())

            @pl.when(s < t)
            def _():
                each_piece(lambda piece: u_hop(s, piece, 1).wait_send())

            return carry

        lax.fori_loop(0, ring, one, 0)

    grad_keys = slope
    slots = [
        lambda: (down_sum.stage(2),),
        lambda: (up_sum.stage(2), down_sum.stage(3)),
        lambda: (up_sum.stage(3), down_sum.stage(4)),
    ]
    for at in reversed(range(blocks)):

        def backward_head(head, carry, at=at):
            query = queries[head, block_rows(at), :]
            grad = grad_context[head, block_rows(at), :]
            spans = key_blocks(at)
            log_total = logs[head, :, block_rows(at)]
            probs = [
                jnp.exp(
                    scores_turned(query, keys, seg_col, segment_row, head, at, span) - log_total
                )
                for span in spans
            ]
            grad_probs = [dot(values[head, block_rows(span), :], grad, 1, 1) for span in spans]
            inner = total(
                [jnp.sum(p * d, axis=0, keepdims=True) for p, d in zip(probs, grad_probs)]
            )
            grad_query = []
            for p, d, span in zip(probs, grad_probs, spans):
                grad_scores = (p * (d - inner)).astype(low)
                grad_value = dot(p.astype(low), grad, 1, 0)
                grad_key = dot(grad_scores, query, 1, 0) * HS ** (-0.5)
                grad_query.append(dot(grad_scores, keys[head, block_rows(span), :], 0, 0))
                if at == min(span + len(key_blocks(blocks)) - 1, blocks - 1):
                    grad_keys[2 * head, block_rows(span), 0:HS] = grad_key
                    grad_keys[2 * head + 1, block_rows(span), 0:HS] = grad_value
                else:
                    grad_keys[2 * head, block_rows(span), 0:HS] += grad_key
                    grad_keys[2 * head + 1, block_rows(span), 0:HS] += grad_value
            grad_q[head] = total(grad_query) * HS ** (-0.5)
            return carry

        lax.fori_loop(0, heads, backward_head, 0)

        per_block = BLOCK // shard
        for piece in reversed(range(per_block)):
            s = at * per_block + piece
            at_rows = slice(s * shard, (s + 1) * shard)
            inside = slice(piece * shard, (piece + 1) * shard)
            cosine = turn_cos[at_rows, :]
            sine = -turn_sin[at_rows, :]
            grads = []
            for index_part in range(3):
                for pair in range(local // LANES):
                    if index_part == 0:
                        halves = [grad_q[2 * pair + e, inside, :] for e in range(2)]
                    else:
                        halves = [
                            grad_keys[2 * (2 * pair + e) + index_part - 1, at_rows, 0:HS]
                            for e in range(2)
                        ]
                    part = jnp.concatenate(halves, axis=1)
                    if index_part < 2:
                        part = turned(part, cosine, sine)
                    grads.append(part.astype(low))
            projected = jnp.concatenate(grads, axis=1)
            grad_proj[at_rows, 0 : 3 * local] = projected
            grad_one = dot(projected, wq[...], 1, 1)
            unit, _ = unit_rows(x_all[at_rows, :].astype(full))
            vectors[0:1, 0:width] += jnp.sum(grad_one * unit, axis=0, keepdims=True)
            vectors[1:2, 0:width] += jnp.sum(grad_one, axis=0, keepdims=True)
            u_all[at_rows, :] += grad_one * gain_one
            u_start(s)
        if slots:
            slots.pop(0)()

    while slots:
        slots.pop(0)()
    for p in branch_hops:
        branch_hop(p)

    def vec_put(slots_ref, base, mine, peer, device):
        return remote(
            vectors,
            slots_ref.at[mine],
            vec_send.at[base + peer],
            vec_recv.at[base + mine],
            **device,
        )

    def vec_round(slots_ref, base, mine, size, device_of):
        others = [lax.rem(mine + step, size) for step in range(1, size)]
        for peer in others:
            vec_put(slots_ref, base, mine, peer, device_of(peer)).start()
        slots_ref[mine] = vectors[...]

        def finish():
            for peer in others:
                vec_put(slots_ref, base, mine, peer, device_of(peer)).wait_send()
                remote(
                    slots_ref.at[peer], slots_ref.at[peer],
                    vec_send.at[base + peer], vec_recv.at[base + peer], tensor=t,
                ).wait_recv()
            vectors[...] = total([slots_ref[index] for index in range(size)])

        return finish

    finish_vec = vec_round(vec_tensor, 0, t, ring, lambda peer: dict(tensor=peer))

    part_mix = part1
    gather_drain(1)
    def out_block(block, carry):
        cols = pl.ds(pl.multiple_of(block * local, local), local)
        part_mix[cols, 3 * local :] = dot(
            heads_side_by_side(context, slice(None)), g_all[:, cols], 0, 0
        ).astype(low)
        return carry

    lax.fori_loop(0, width // local, out_block, 0)

    def norm_again(s, carry):
        unit, _ = unit_rows(x_all[rows(s), :].astype(full))
        g_all[rows(s), :] = (unit * gain_one + shift_one).astype(low)
        return carry

    lax.fori_loop(0, ring, norm_again, 0)
    def mix_block(block, carry):
        span = pl.ds(pl.multiple_of(block * BLOCK, BLOCK), BLOCK)
        part_mix[span, 0 : 3 * local] = dot(
            g_all[:, span], grad_proj[:, 0 : 3 * local], 0, 0
        ).astype(low)
        return carry

    lax.fori_loop(0, width // BLOCK, mix_block, 0)
    mix_sum = DataSum(
        spots, (part_mix, done2, half2, a12, b12, a22, b22), data_send.at[2], data_recv.at[2]
    )
    mix_sum.stage(0)
    last_tick = (PIECES + 2) * ring - 6

    def ticks(share_from, share_to):
        u_steps(last_tick * share_from // 18, last_tick * share_to // 18)

    up_sum.stage(4)
    ticks(0, 9)
    mix_sum.stage(1)
    down_sum.stage(5)
    finish_vec()
    finish_vec = vec_round(
        vec_core, ring, core, 2, lambda peer: dict(dp=dp_of(peer, x_at, y_at))
    )
    ticks(9, 12)
    up_sum.stage(5)
    mix_sum.stage(2)
    finish_vec()
    finish_vec = vec_round(
        vec_x, ring + 2, x_at, nx, lambda peer: dict(dp=dp_of(core, peer, y_at))
    )
    down_sum.stage(6)
    copies = [pltpu.make_async_copy(done0, grad_down_out, out_sem.at[0])]
    copies[-1].start()
    ticks(12, 15)
    mix_sum.stage(3)
    up_sum.stage(6)
    copies.append(pltpu.make_async_copy(done1, grad_up_out, out_sem.at[1]))
    copies[-1].start()
    finish_vec()
    finish_vec = vec_round(
        vec_y, ring + 2 + nx, y_at, 2, lambda peer: dict(dp=dp_of(core, x_at, peer))
    )
    ticks(15, 18)
    mix_sum.stage(4)
    branch_buf[t] = (x_all[rows(t), :].astype(full) + branch_own()).astype(low)
    copies.append(pltpu.make_async_copy(branch_buf.at[t], output_rows, out_sem.at[2]))
    copies[-1].start()
    own_cotangent = branch_buf.at[ring]
    own_load = pltpu.make_async_copy(cotangent, own_cotangent, load_sem.at[0])
    own_load.start()
    finish_vec()
    rows_all = group * ranks
    rms_active = jnp.sqrt(jnp.sum(vectors[4:5, :], axis=1, keepdims=True) / (rows_all * FF))
    rms_context = jnp.sqrt(jnp.sum(vectors[5:6, :], axis=1, keepdims=True) / (rows_all * width))
    vectors_out[0:4, :] = vectors[0:4, :]
    vectors_out[4:5, :] = jnp.broadcast_to(rms_context, (1, vectors.shape[1]))
    vectors_out[5:6, :] = jnp.broadcast_to(rms_active, (1, vectors.shape[1]))
    vectors_out[6:8, :] = jnp.zeros_like(vectors_out[6:8, :])
    weighted = u_own()
    own_load.wait()
    unit, scale = unit_rows(x_all[rows(t), :].astype(full))
    grad_rows = scale * (
        weighted
        - jnp.mean(weighted, axis=-1, keepdims=True)
        - unit * jnp.mean(weighted * unit, axis=-1, keepdims=True)
    )
    grad_buf[t] = (own_cotangent[...].astype(full) + grad_rows).astype(low)
    copies.append(pltpu.make_async_copy(grad_buf.at[t], input_grad, out_sem.at[3]))
    copies[-1].start()
    mix_sum.stage(5)
    mix_sum.stage(6)
    for part in range(3):
        copies.append(
            pltpu.make_async_copy(
                done2.at[:, part * local : (part + 1) * local],
                grad_qkv_out.at[part],
                out_sem.at[4 + part],
            )
        )
        copies[-1].start()
    for block in range(width // local):
        cols = slice(block * local, (block + 1) * local)
        copies.append(
            pltpu.make_async_copy(
                done2.at[cols, 3 * local :], grad_out_out.at[:, cols], out_sem.at[7 + block]
            )
        )
        copies[-1].start()
    gather_drain(0)
    branch_drain()
    u_drain()
    for copy in copies:
        copy.wait()


def widen_kernel(*refs):
    count = 6
    for source, target in zip(refs[:count], refs[count + 1 : 2 * count + 1]):
        target[...] = source[...].astype(target.dtype)
    vectors = refs[count]
    for index, target in enumerate(refs[2 * count + 1 :]):
        target[...] = vectors[index : index + 1, 0 : target.shape[1]]


def widen(arrays, vectors, width):
    steps = 8

    def spec(shape):
        block = list(shape)
        block[-2] //= steps
        lead = (0,) * (len(shape) - 2)
        return pl.BlockSpec(tuple(block), lambda i, lead=lead: (*lead, i, 0))

    kinds = [low, low, full, full, full, full]
    small = [(1, width)] * 4 + [(1, 1)] * 2
    whole = lambda shape: pl.BlockSpec(shape, lambda i: (0, 0))
    return pl.pallas_call(
        widen_kernel,
        name="widen",
        grid=(steps,),
        out_shape=[jax.ShapeDtypeStruct(a.shape, kind) for a, kind in zip(arrays, kinds)]
        + [jax.ShapeDtypeStruct(shape, full) for shape in small],
        in_specs=[spec(a.shape) for a in arrays] + [whole(vectors.shape)],
        out_specs=[spec(a.shape) for a in arrays] + [whole(shape) for shape in small],
    )(*arrays, vectors)


def per_device(
    ring, ranks,
    tokens, segments, w_qkv, w_out, w_up, w_down,
    gain_one, shift_one, gain_two, shift_two, cotangent,
):
    shard, width = tokens.shape
    group = segments.shape[1]
    local = w_qkv.shape[2]
    heads = local // HS
    hidden_local = w_up.shape[1]
    nx = ranks // 4
    half_rot = ROT // 2
    lane = np.arange(LANES) % HS
    frequency = rotary_base ** (-(2.0 * (lane % half_rot)) / ROT)
    frequency = np.where(lane < ROT, frequency, 0.0)
    sign = np.where(lane < half_rot, -1.0, 1.0)
    table = jnp.asarray(np.stack([frequency, sign] + [np.zeros(LANES)] * 6), jnp.float32)
    vmem = pl.BlockSpec(memory_space=pltpu.VMEM)
    anywhere = pl.BlockSpec(memory_space=pl.ANY)
    wide = max(width, hidden_local)
    scratch = lambda *shape: pltpu.VMEM(shape, low)
    wider = lambda *shape: pltpu.VMEM(shape, full)
    sems = lambda *shape: pltpu.SemaphoreType.DMA(shape)

    def sum_buffers(rows, columns):
        return [
            scratch(rows, columns),
            scratch(rows, columns),
            scratch(rows // 2, columns),
            scratch(nx - 1, rows // (4 * nx), columns),
            scratch(1, rows // 8, columns),
            scratch(1, rows // (8 * nx), columns),
            scratch(nx - 1, rows // (8 * nx), columns),
        ]

    data_sems = 12 + 4 * nx
    outs = pl.pallas_call(
        partial(layer_kernel, ring, ranks),
        name="layer",
        out_shape=[
            jax.ShapeDtypeStruct((shard, width), low),
            jax.ShapeDtypeStruct((shard, width), low),
            jax.ShapeDtypeStruct((hidden_local, width), low),
            jax.ShapeDtypeStruct((width, hidden_local), low),
            jax.ShapeDtypeStruct((3, width, local), low),
            jax.ShapeDtypeStruct((local, width), low),
            jax.ShapeDtypeStruct((8, wide), full),
        ],
        in_specs=[anywhere] * 2 + [vmem] * 6 + [anywhere] * 4,
        out_specs=[anywhere] * 6 + [vmem],
        scratch_shapes=[
            scratch(width, 3 * local), scratch(local, width),
            scratch(width, hidden_local), scratch(hidden_local, width),
            sems(8), sems(7 + width // local),
            wider(group, 1),
            scratch(group, width), scratch(group, width), scratch(group, width),
            scratch(group, hidden_local),
            wider(hidden_local // LANES, group, LANES),
            wider(group, width),
            wider(hidden_local, width), wider(width, hidden_local),
            scratch(heads, group, HS), scratch(heads, group, HS), scratch(heads, group, HS),
            scratch(heads, group, HS), scratch(heads, group, HS),
            wider(heads, 1, group),
            wider(heads, BLOCK, HS),
            wider(group, LANES), wider(group, LANES),
            sems(2, 2, ring), sems(2, ring),
            scratch(ring + 1, shard, width), sems(ring), sems(ring + 1),
            scratch(ring + 1, shard, width), sems(ring, PIECES), sems(ring + 1, PIECES),
            *sum_buffers(hidden_local, width),
            *sum_buffers(width, hidden_local)[1:],
            *sum_buffers(width, 4 * local)[1:],
            sems(3, data_sems), sems(3, data_sems),
            wider(8, wide), wider(ring, 8, wide), wider(2, 8, wide),
            wider(nx, 8, wide), wider(2, 8, wide),
            sems(ring + 4 + nx), sems(ring + 4 + nx),
        ],
        compiler_params=pltpu.CompilerParams(
            collective_id=0, has_side_effects=True, vmem_limit_bytes=67043328
        ),
    )(
        tokens, cotangent, segments,
        *(v.reshape(1, width) for v in (gain_one, shift_one, gain_two, shift_two)), table,
        w_qkv.transpose(1, 0, 2), w_out, w_up, w_down,
    )
    output_rows, input_grad, grad_down, grad_up, grad_qkv, grad_out, *small = widen(
        outs[:6], outs[6], width
    )
    return (
        output_rows,
        input_grad,
        grad_qkv.transpose(1, 0, 2),
        grad_out,
        grad_up,
        grad_down,
        *(v.reshape(width) for v in small[:4]),
        small[4].reshape(()),
        small[5].reshape(()),
    )


def solution(mesh):
    everyone = P(("dp", "tensor"), None)
    return jax.shard_map(
        partial(per_device, mesh.shape["tensor"], mesh.shape["dp"]),
        mesh=mesh,
        in_specs=(
            everyone,
            P("dp", None),
            P(None, None, "tensor"),
            P("tensor", None),
            P(None, "tensor"),
            P("tensor", None),
            P(),
            P(),
            P(),
            P(),
            everyone,
        ),
        out_specs=(
            everyone,
            everyone,
            P(None, None, "tensor"),
            P("tensor", None),
            P(None, "tensor"),
            P("tensor", None),
            P(),
            P(),
            P(),
            P(),
            P(),
            P(),
        ),
        check_vma=False,
    )
```

```python
from functools import partial, reduce

import jax
import jax.numpy as jnp
import numpy as np
from jax import lax
from jax.experimental import pallas as pl
from jax.experimental.pallas import tpu as pltpu
from jax.sharding import PartitionSpec as P

HS = 64
ROT = 16
FF = 4096
BLOCK = 256
LONGEST = 512
LANES = 128
PIECES = 2

epsilon = 1e-05
rotary_base = 10000.0
masked_score = -1000000000.0
low = jnp.bfloat16
full = jnp.float32
MESH = pl.DeviceIdType.MESH


def dot(a, b, over_a, over_b):
    return lax.dot_general(
        a, b, (((over_a,), (over_b,)), ((), ())), preferred_element_type=jnp.float32
    )


def total(parts):
    return reduce(jnp.add, parts)


def unit_rows(values):
    average = jnp.mean(values, axis=-1, keepdims=True)
    centred = values - average
    variance = jnp.mean(centred * centred, axis=-1, keepdims=True)
    scale = lax.rsqrt(variance + epsilon)
    return centred * scale, scale


def block_rows(index):
    return slice(index * BLOCK, (index + 1) * BLOCK)


def key_blocks(index):
    reach = (LONGEST + BLOCK - 2) // BLOCK
    return range(max(0, index - reach), index + 1)


def scores_turned(query, keys, seg_col, segment_row, head, at, key_at):
    scores = dot(keys[head, block_rows(key_at), :], query, 1, 1) * HS ** (-0.5)
    allowed = seg_col[block_rows(key_at), :] == segment_row[:, block_rows(at)]
    if at == key_at:
        key_index = lax.broadcasted_iota(jnp.int32, (BLOCK, BLOCK), 0)
        query_index = lax.broadcasted_iota(jnp.int32, (BLOCK, BLOCK), 1)
        allowed = allowed & (key_index <= query_index)
    return jnp.where(allowed, scores, masked_score)


def remote(source, target, send, receive, **device):
    return pltpu.make_async_remote_copy(
        source, target, send, receive, device_id=device, device_id_type=MESH
    )


class DataSum:
    def __init__(self, spots, bufs, send, receive):
        self.part, self.done, self.half, self.a1, self.b1, self.a2, self.b2 = bufs
        self.core, self.x, self.y, self.nx = spots
        self.send, self.receive = send, receive
        rows = self.part.shape[0]
        self.rows = rows
        self.open = []

    def dp(self, core=None, x=None, y=None):
        core = self.core if core is None else core
        x = self.x if x is None else x
        y = self.y if y is None else y
        return (y * self.nx + x) * 2 + core

    def rows_at(self, start, size):
        return pl.ds(pl.multiple_of(start, size), size)

    def put(self, source, target, base, mine, peer, device):
        copy = remote(
            source, target, self.send.at[base + peer], self.receive.at[base + mine], dp=device
        )
        copy.start()
        self.open.append(copy)

    def take(self, target, base, peer):
        remote(
            target, target, self.send.at[base + peer], self.receive.at[base + peer],
            dp=self.dp(),
        ).wait_recv()

    def drain(self):
        for copy in self.open:
            copy.wait_send()
        self.open = []

    def seat(self, sender, receiver):
        return lax.rem(sender - receiver - 1 + 2 * self.nx, self.nx)

    def x_peers(self):
        return [lax.rem(self.x + step, self.nx) for step in range(1, self.nx)]

    def bases(self):
        nx = self.nx
        names = {}
        at = 0
        for name, size in (
            ("c", 2), ("a1", nx), ("b1", 2), ("a2", 2), ("b2", nx),
            ("a3", 2), ("b3", nx), ("a4", nx), ("b4", 2), ("d", 2),
        ):
            names[name] = at
            at += size
        names["all"] = at
        return names

    def stage(self, number):
        rows, nx, core, x, y = self.rows, self.nx, self.core, self.x, self.y
        base = self.bases()
        half, quarter, eighth = rows // 2, rows // 4, rows // 8
        a_size, b_size, tail = quarter // nx, eighth, eighth // nx
        other, across = 1 - core, 1 - y
        start = core * half
        if number == 0:
            self.put(
                self.part.at[self.rows_at(other * half, half), :], self.half,
                base["c"], core, other, self.dp(core=other),
            )
        if number == 1:
            self.take(self.half, base["c"], other)
            add_rows(
                self.half, 0, [(self.part, start), (self.half, 0)], half
            )
            self.drain()
            for peer in self.x_peers():
                self.put(
                    self.half.at[self.rows_at(peer * a_size, a_size), :], self.a1.at[self.seat(x, peer)],
                    base["a1"], x, peer, self.dp(x=peer),
                )
            self.put(
                self.half.at[self.rows_at(quarter + across * b_size, b_size), :], self.b1.at[0],
                base["b1"], y, across, self.dp(y=across),
            )
        if number == 2:
            for peer in self.x_peers():
                self.take(self.a1.at[self.seat(peer, x)], base["a1"], peer)
            add_rows(
                self.half, x * a_size,
                [(self.half, x * a_size)] + [(self.a1.at[self.seat(peer, x)], 0) for peer in self.x_peers()],
                a_size,
            )
            self.take(self.b1.at[0], base["b1"], across)
            add_rows(
                self.half, quarter + y * b_size,
                [(self.half, quarter + y * b_size), (self.b1.at[0], 0)],
                b_size,
            )
            self.drain()
            self.put(
                self.half.at[self.rows_at(x * a_size + across * tail, tail), :], self.a2.at[0],
                base["a2"], y, across, self.dp(y=across),
            )
            for peer in self.x_peers():
                self.put(
                    self.half.at[self.rows_at(quarter + y * b_size + peer * tail, tail), :],
                    self.b2.at[self.seat(x, peer)], base["b2"], x, peer, self.dp(x=peer),
                )
        if number == 3:
            a_own = x * a_size + y * tail
            b_own = quarter + y * b_size + x * tail
            self.take(self.a2.at[0], base["a2"], across)
            add_rows(
                self.done, start + a_own, [(self.half, a_own), (self.a2.at[0], 0)], tail
            )
            for peer in self.x_peers():
                self.take(self.b2.at[self.seat(peer, x)], base["b2"], peer)
            add_rows(
                self.done, start + b_own,
                [(self.half, b_own)] + [(self.b2.at[self.seat(peer, x)], 0) for peer in self.x_peers()],
                tail,
            )
            self.drain()
            piece = self.done.at[self.rows_at(start + a_own, tail), :]
            self.put(piece, piece, base["a3"], y, across, self.dp(y=across))
            piece = self.done.at[self.rows_at(start + b_own, tail), :]
            for peer in self.x_peers():
                self.put(piece, piece, base["b3"], x, peer, self.dp(x=peer))
        if number == 4:
            self.take(
                self.done.at[self.rows_at(start + x * a_size + across * tail, tail), :],
                base["a3"], across,
            )
            for peer in self.x_peers():
                self.take(
                    self.done.at[
                        self.rows_at(start + quarter + y * b_size + peer * tail, tail), :
                    ],
                    base["b3"], peer,
                )
            self.drain()
            piece = self.done.at[self.rows_at(start + x * a_size, a_size), :]
            for peer in self.x_peers():
                self.put(piece, piece, base["a4"], x, peer, self.dp(x=peer))
            piece = self.done.at[self.rows_at(start + quarter + y * b_size, b_size), :]
            self.put(piece, piece, base["b4"], y, across, self.dp(y=across))
        if number == 5:
            for peer in self.x_peers():
                self.take(
                    self.done.at[self.rows_at(start + peer * a_size, a_size), :],
                    base["a4"], peer,
                )
            self.take(
                self.done.at[self.rows_at(start + quarter + across * b_size, b_size), :],
                base["b4"], across,
            )
            self.drain()
            piece = self.done.at[self.rows_at(start, half), :]
            self.put(piece, piece, base["d"], core, other, self.dp(core=other))
        if number == 6:
            self.take(self.done.at[self.rows_at(other * half, half), :], base["d"], other)
            self.drain()


def add_rows(target, target_start, sources, size):
    step = min(size, 64)

    def one(index, carry):
        offset = index * step

        def rows(start):
            return pl.ds(pl.multiple_of(start + offset, min(step, 16)), step)

        summed = total([ref[rows(start), :].astype(full) for ref, start in sources])
        target[rows(target_start), :] = summed.astype(target.dtype)
        return carry

    lax.fori_loop(0, size // step, one, 0)


def layer_kernel(
    ring,
    ranks,
    tokens, cotangent, seg_row, gains_one, shifts_one, gains_two, shifts_two, table,
    w_qkv, w_out, w_up, w_down,
    output_rows, input_grad, grad_down_out, grad_up_out, grad_qkv_out, grad_out_out, vectors_out,
    wq, wo, wu, wd, load_sem, out_sem,
    seg_col, x_all, g_all, normed_two, active, slope, u_all,
    acc_down, acc_up, queries, keys, values, grad_context, context, logs,
    grad_q, turn_cos, turn_sin,
    gather_send, gather_recv,
    branch_buf, branch_send, branch_recv, grad_buf, grad_send, grad_recv,
    part0, done0, half0, a10, b10, a20, b20,
    done1, half1, a11, b11, a21, b21,
    done2, half2, a12, b12, a22, b22,
    data_send, data_recv,
    vectors, vec_tensor, vec_core, vec_x, vec_y, vec_send, vec_recv,
):
    group = x_all.shape[0]
    width = x_all.shape[1]
    shard = group // ring
    heads = queries.shape[0]
    local = heads * HS
    blocks = group // BLOCK
    hidden_local = wu.shape[1]
    hidden_part = min(hidden_local, BLOCK)
    nx = ranks // 4
    part1 = wu
    grad_proj = normed_two
    t = lax.axis_index("tensor")
    dp = lax.axis_index("dp")
    core = lax.rem(dp, 2)
    x_at = lax.rem(dp // 2, nx)
    y_at = dp // (2 * nx)
    spots = (core, x_at, y_at, nx)

    def rows(s):
        return pl.ds(pl.multiple_of(s * shard, shard), shard)

    def dp_of(c, x, y):
        return (y * nx + x) * 2 + c

    pairs = [(tokens, x_all.at[rows(t), :]), (cotangent, g_all.at[rows(t), :])]
    pairs += [
        (w_qkv.at[part], wq.at[:, part * local : (part + 1) * local]) for part in range(3)
    ]
    pairs += [(w_up, wu), (w_out, wo), (w_down, wd)]
    loads = [
        pltpu.make_async_copy(source, target, load_sem.at[index])
        for index, (source, target) in enumerate(pairs)
    ]
    for copy in loads:
        copy.start()

    barrier = pltpu.get_barrier_semaphore()
    peers = [dict(tensor=lax.rem(t + step, ring)) for step in range(1, ring)]
    peers.append(dict(dp=dp_of(1 - core, x_at, y_at)))
    peers.append(dict(dp=dp_of(core, x_at, 1 - y_at)))
    for step in range(1, nx):
        peers.append(dict(dp=dp_of(core, lax.rem(x_at + step, nx), y_at)))
    for peer in peers:
        pl.semaphore_signal(barrier, inc=1, device_id=peer, device_id_type=MESH)
    pl.semaphore_wait(barrier, len(peers))

    def relay(which, source, s, side):
        target = (x_all, g_all)[which].at[rows(s), :]
        return remote(
            source,
            target,
            gather_send.at[which, side, s],
            gather_recv.at[which, s],
            tensor=t + 1 if side == 0 else t - 1,
        )

    def arrive(which, s):
        target = (x_all, g_all)[which].at[rows(s), :]
        remote(
            target, target, gather_send.at[which, 0, s], gather_recv.at[which, s], tensor=t
        ).wait_recv()

    def gather_step(which, k):
        array = (x_all, g_all)[which]

        @pl.when((k > 0) & (t - k >= 0))
        def _():
            s = t - k
            arrive(which, s)

            @pl.when(t < ring - 1)
            def _():
                relay(which, array.at[rows(s), :], s, 0).start()

        @pl.when((k > 0) & (t + k < ring))
        def _():
            s = t + k
            arrive(which, s)

            @pl.when(t > 0)
            def _():
                relay(which, array.at[rows(s), :], s, 1).start()

    def gather_own(which, side):
        relay(which, (tokens, cotangent)[which], t, side).start()

    def gather_drain(which):
        array = (x_all, g_all)[which]

        def one(s, carry):
            @pl.when((s <= t) & (t < ring - 1))
            def _():
                relay(which, array.at[rows(s), :], s, 0).wait_send()

            @pl.when((s >= t) & (t > 0))
            def _():
                relay(which, array.at[rows(s), :], s, 1).wait_send()

            return carry

        lax.fori_loop(0, ring, one, 0)

    @pl.when(t < ring - 1)
    def _():
        gather_own(0, 0)

    @pl.when(t > 0)
    def _():
        gather_own(0, 1)

    segment_row = seg_row[...].astype(full)
    seg_col[...] = jnp.broadcast_to(segment_row, (LANES, group)).T[:, 0:1]
    vectors[...] = jnp.zeros_like(vectors)
    acc_down[...] = jnp.zeros_like(acc_down)
    acc_up[...] = jnp.zeros_like(acc_up)
    gain_one, shift_one = gains_one[...], shifts_one[...]
    gain_two, shift_two = gains_two[...], shifts_two[...]
    for copy in loads:
        copy.wait()

    lane = lax.broadcasted_iota(jnp.int32, (shard, LANES), 1) % HS

    def turned(part, cosine, sine):
        moved = jnp.where(
            lane < ROT // 2, pltpu.roll(part, LANES - ROT // 2, 1), pltpu.roll(part, ROT // 2, 1)
        )
        return part * cosine + moved * sine

    def forward_rows(s):
        at = rows(s)
        unit, _ = unit_rows(x_all[at, :].astype(full))
        one = (unit * gain_one + shift_one).astype(low)
        two = (unit * gain_two + shift_two).astype(low)
        normed_two[at, :] = two
        own_segments = seg_col[at, :]
        before = jnp.sum((segment_row < own_segments).astype(jnp.int32), axis=1, keepdims=True)
        index = lax.broadcasted_iota(jnp.int32, (shard, 1), 0) + s * shard
        position = (index - before).astype(full)
        angle = position * table[0:1, :]
        cosine = jnp.cos(angle)
        sine = jnp.sin(angle) * table[1:2, :]
        turn_cos[at, :] = cosine
        turn_sin[at, :] = sine
        projected = dot(one, wq[...], 1, 0)
        for index_part, ref in enumerate((queries, keys, values)):
            for pair in range(local // LANES):
                lo = index_part * local + pair * LANES
                part = projected[:, lo : lo + LANES]
                if index_part < 2:
                    part = turned(part, cosine, sine)
                part = part.astype(low)
                for side in range(LANES // HS):
                    ref[pair * (LANES // HS) + side, at, :] = part[:, side * HS : (side + 1) * HS]
        for lo in range(0, hidden_local, hidden_part):
            span = slice(lo, lo + hidden_part)
            hidden = dot(two, wu[:, span], 1, 0)
            inner = 0.5 * (1.0 + lax.erf(hidden * 0.7071067811865476))
            activated = hidden * inner
            steep = inner + hidden * jnp.exp(-0.5 * hidden * hidden) * 0.3989422804014327
            active[at, span] = activated.astype(low)
            for chunk in range(hidden_part // LANES):
                slope[lo // LANES + chunk, at, :] = steep[:, chunk * LANES : (chunk + 1) * LANES]
            vectors[4:5, span] += jnp.sum(activated * activated, axis=0, keepdims=True)

    def both_sides(k, body):
        def one(side, carry):
            s = jnp.where(side == 0, t - k, t + k)

            @pl.when((s >= 0) & (s < ring) & ((k > 0) | (side == 0)))
            def _():
                body(s)

            return carry

        lax.fori_loop(0, 2, one, 0)

    def forward_step(k, carry):
        gather_step(0, k)

        @pl.when((k == t) & (t < ring - 1))
        def _():
            gather_own(1, 0)

        @pl.when((k == ring - 1 - t) & (t > 0))
        def _():
            gather_own(1, 1)

        both_sides(k, forward_rows)
        return carry

    lax.fori_loop(0, ring, forward_step, 0)

    for at in range(blocks):

        def forward_head(head, carry, at=at):
            query = queries[head, block_rows(at), :]
            spans = key_blocks(at)
            scores = [
                scores_turned(query, keys, seg_col, segment_row, head, at, span) for span in spans
            ]
            most = reduce(jnp.maximum, [jnp.max(s, axis=0, keepdims=True) for s in scores])
            raised = [jnp.exp(s - most) for s in scores]
            summed = total([jnp.sum(e, axis=0, keepdims=True) for e in raised])
            share = 1.0 / summed
            logs[head, :, block_rows(at)] = most + jnp.log(summed)
            mixed = total(
                [
                    dot((e * share).astype(low), values[head, block_rows(span), :], 0, 0)
                    for e, span in zip(raised, spans)
                ]
            )
            context[head, block_rows(at), :] = mixed.astype(low)
            vectors[5:6, 0:HS] += jnp.sum(mixed * mixed, axis=0, keepdims=True)
            return carry

        lax.fori_loop(0, heads, forward_head, 0)

    def heads_side_by_side(ref, at):
        return jnp.concatenate([ref[head, at, :] for head in range(heads)], axis=1)

    def branch_rows(s):
        at = rows(s)
        return dot(heads_side_by_side(context, at), wo[...], 1, 0) + dot(
            active[at, :], wd[...], 1, 0
        )

    def chain(buffer, send, receive, make):
        def hop(s, side):
            if side == 0:
                slot = s
            else:
                slot = jnp.where(s == t - 1, ring, s)
            return remote(
                buffer.at[s],
                buffer.at[slot],
                send.at[s],
                receive.at[slot],
                tensor=t + 1 if side == 0 else t - 1,
            )

        def landed(slot):
            remote(buffer.at[slot], buffer.at[slot], send.at[0], receive.at[slot], tensor=t).wait_recv()

        def pass_on(s, side):
            has = t > 0 if side == 0 else t < ring - 1

            @pl.when(has)
            def _():
                landed(s)
                buffer[s] = (make(s) + buffer[s].astype(full)).astype(low)

            @pl.when(jnp.logical_not(has))
            def _():
                buffer[s] = make(s).astype(low)

            hop(s, side).start()

        def own():
            value = make(t)

            @pl.when(t > 0)
            def _():
                landed(t)

            @pl.when(t < ring - 1)
            def _():
                landed(ring)

            left = jnp.where(t > 0, buffer[t].astype(full), 0.0)
            right = jnp.where(t < ring - 1, buffer[ring].astype(full), 0.0)
            return value + left + right

        def drain():
            def one(s, carry):
                @pl.when(s > t)
                def _():
                    hop(s, 0).wait_send()

                @pl.when(s < t)
                def _():
                    hop(s, 1).wait_send()

                return carry

            lax.fori_loop(0, ring, one, 0)

        return pass_on, own, drain

    branch_pass, branch_own, branch_drain = chain(
        branch_buf, branch_send, branch_recv, branch_rows
    )

    def backward_rows(s):
        at = rows(s)
        grad = g_all[at, :]
        grad_two = None
        for lo in range(0, hidden_local, hidden_part):
            span = slice(lo, lo + hidden_part)
            steep = jnp.concatenate(
                [slope[lo // LANES + chunk, at, :] for chunk in range(hidden_part // LANES)],
                axis=1,
            )
            grad_hidden = (dot(grad, wd[span, :], 1, 1) * steep).astype(low)
            acc_down[span, :] += dot(active[at, span], grad, 0, 0)
            acc_up[:, span] += dot(normed_two[at, :], grad_hidden, 0, 0)
            more = dot(grad_hidden, wu[:, span], 1, 1)
            grad_two = more if grad_two is None else grad_two + more
        unit, _ = unit_rows(x_all[at, :].astype(full))
        vectors[2:3, 0:width] += jnp.sum(grad_two * unit, axis=0, keepdims=True)
        vectors[3:4, 0:width] += jnp.sum(grad_two, axis=0, keepdims=True)
        u_all[at, :] = grad_two * gain_two
        back = dot(grad, wo[...], 1, 1).astype(low)
        for head in range(heads):
            grad_context[head, at, :] = back[:, head * HS : (head + 1) * HS]

    def backward_step(k, carry):
        gather_step(1, k)

        @pl.when((t == 0) & (k < ring - 1))
        def _():
            branch_pass(ring - 1 - k, 0)

        @pl.when((t == ring - 1) & (k < ring - 1))
        def _():
            branch_pass(k, 1)

        both_sides(k, backward_rows)
        return carry

    lax.fori_loop(0, ring, backward_step, 0)

    def narrow(source, target):
        step = 64

        def one(index, carry):
            at = pl.ds(pl.multiple_of(index * step, step), step)
            target[at, :] = source[at, :].astype(low)
            return carry

        lax.fori_loop(0, source.shape[0] // step, one, 0)

    down_sum = DataSum(
        spots, (part0, done0, half0, a10, b10, a20, b20), data_send.at[0], data_recv.at[0]
    )
    up_sum = DataSum(
        spots, (part1, done1, half1, a11, b11, a21, b21), data_send.at[1], data_recv.at[1]
    )
    def branch_hop(p):
        s_up = ring - 2 - p + t

        @pl.when((t > 0) & (s_up > t) & (s_up < ring))
        def _():
            branch_pass(s_up, 0)

        s_down = p + 2 - ring + t

        @pl.when((t < ring - 1) & (s_down >= 0) & (s_down < t))
        def _():
            branch_pass(s_down, 1)

    narrow(acc_down, part0)
    down_sum.stage(0)
    narrow(acc_up, part1)
    up_sum.stage(0)
    branch_hop(0)
    branch_hops = list(range(1, ring - 2))
    down_sum.stage(1)
    up_sum.stage(1)

    part_rows = shard // PIECES

    def u_hop(s, piece, side):
        at = pl.ds(pl.multiple_of(piece * part_rows, part_rows), part_rows)
        slot = s if side == 0 else jnp.where(s == t - 1, ring, s)
        return remote(
            grad_buf.at[s, at, :],
            grad_buf.at[slot, at, :],
            grad_send.at[s, piece],
            grad_recv.at[slot, piece],
            tensor=t + 1 if side == 0 else t - 1,
        )

    def u_landed(slot, piece):
        at = pl.ds(pl.multiple_of(piece * part_rows, part_rows), part_rows)
        ref = grad_buf.at[slot, at, :]
        remote(ref, ref, grad_send.at[0, piece], grad_recv.at[slot, piece], tensor=t).wait_recv()

    def each_piece(body):
        def one(piece, carry):
            body(piece)
            return carry

        lax.fori_loop(0, PIECES, one, 0)

    def u_start(s):
        for side, end in ((0, 0), (1, ring - 1)):
            if s == end:
                continue

            @pl.when(t == end)
            def _(side=side):
                grad_buf[s] = u_all[rows(s), :].astype(low)
                each_piece(lambda piece: u_hop(s, piece, side).start())

    def u_pass(s, piece, side):
        u_landed(s, piece)
        at = pl.ds(pl.multiple_of(piece * part_rows, part_rows), part_rows)
        source = pl.ds(pl.multiple_of(s * shard + piece * part_rows, part_rows), part_rows)
        grad_buf[s, at, :] = (u_all[source, :] + grad_buf[s, at, :].astype(full)).astype(low)
        u_hop(s, piece, side).start()

    def u_step(tick, carry):
        up = tick - 2 * t
        s_up = ring - 1 - up // PIECES

        @pl.when((t > 0) & (up >= 0) & (s_up > t))
        def _():
            u_pass(s_up, lax.rem(up, PIECES), 0)

        down = tick + 2 - 2 * (ring - 1 - t)
        s_down = ring - 1 - down // PIECES

        @pl.when((t < ring - 1) & (down >= 0) & (s_down >= 0) & (s_down < t))
        def _():
            u_pass(s_down, lax.rem(down, PIECES), 1)

        return carry

    def u_steps(first, last):
        lax.fori_loop(first, last, u_step, 0)

    def u_own():
        @pl.when(t > 0)
        def _():
            each_piece(lambda piece: u_landed(t, piece))

        @pl.when(t < ring - 1)
        def _():
            each_piece(lambda piece: u_landed(ring, piece))

        left = jnp.where(t > 0, grad_buf[t].astype(full), 0.0)
        right = jnp.where(t < ring - 1, grad_buf[ring].astype(full), 0.0)
        return u_all[rows(t), :] + left + right

    def u_drain():
        def one(s, carry):
            @pl.when(s > t)
            def _():
                each_piece(lambda piece: u_hop(s, piece, 0).wait_send())

            @pl.when(s < t)
            def _():
                each_piece(lambda piece: u_hop(s, piece, 1).wait_send())

            return carry

        lax.fori_loop(0, ring, one, 0)

    grad_keys = slope
    slots = [
        lambda: (down_sum.stage(2),),
        lambda: (up_sum.stage(2), down_sum.stage(3)),
        lambda: (up_sum.stage(3), down_sum.stage(4)),
    ]
    for at in reversed(range(blocks)):

        def backward_head(head, carry, at=at):
            query = queries[head, block_rows(at), :]
            grad = grad_context[head, block_rows(at), :]
            spans = key_blocks(at)
            log_total = logs[head, :, block_rows(at)]
            probs = [
                jnp.exp(
                    scores_turned(query, keys, seg_col, segment_row, head, at, span) - log_total
                )
                for span in spans
            ]
            grad_probs = [dot(values[head, block_rows(span), :], grad, 1, 1) for span in spans]
            inner = total(
                [jnp.sum(p * d, axis=0, keepdims=True) for p, d in zip(probs, grad_probs)]
            )
            grad_query = []
            for p, d, span in zip(probs, grad_probs, spans):
                grad_scores = (p * (d - inner)).astype(low)
                grad_value = dot(p.astype(low), grad, 1, 0)
                grad_key = dot(grad_scores, query, 1, 0) * HS ** (-0.5)
                grad_query.append(dot(grad_scores, keys[head, block_rows(span), :], 0, 0))
                if at == min(span + len(key_blocks(blocks)) - 1, blocks - 1):
                    grad_keys[2 * head, block_rows(span), 0:HS] = grad_key
                    grad_keys[2 * head + 1, block_rows(span), 0:HS] = grad_value
                else:
                    grad_keys[2 * head, block_rows(span), 0:HS] += grad_key
                    grad_keys[2 * head + 1, block_rows(span), 0:HS] += grad_value
            grad_q[head] = total(grad_query) * HS ** (-0.5)
            return carry

        lax.fori_loop(0, heads, backward_head, 0)

        per_block = BLOCK // shard
        for piece in reversed(range(per_block)):
            s = at * per_block + piece
            at_rows = slice(s * shard, (s + 1) * shard)
            inside = slice(piece * shard, (piece + 1) * shard)
            cosine = turn_cos[at_rows, :]
            sine = -turn_sin[at_rows, :]
            grads = []
            for index_part in range(3):
                for pair in range(local // LANES):
                    if index_part == 0:
                        halves = [grad_q[2 * pair + e, inside, :] for e in range(2)]
                    else:
                        halves = [
                            grad_keys[2 * (2 * pair + e) + index_part - 1, at_rows, 0:HS]
                            for e in range(2)
                        ]
                    part = jnp.concatenate(halves, axis=1)
                    if index_part < 2:
                        part = turned(part, cosine, sine)
                    grads.append(part.astype(low))
            projected = jnp.concatenate(grads, axis=1)
            grad_proj[at_rows, 0 : 3 * local] = projected
            grad_one = dot(projected, wq[...], 1, 1)
            unit, _ = unit_rows(x_all[at_rows, :].astype(full))
            vectors[0:1, 0:width] += jnp.sum(grad_one * unit, axis=0, keepdims=True)
            vectors[1:2, 0:width] += jnp.sum(grad_one, axis=0, keepdims=True)
            u_all[at_rows, :] += grad_one * gain_one
            u_start(s)
        if slots:
            slots.pop(0)()

    while slots:
        slots.pop(0)()
    for p in branch_hops:
        branch_hop(p)

    def vec_put(slots_ref, base, mine, peer, device):
        return remote(
            vectors,
            slots_ref.at[mine],
            vec_send.at[base + peer],
            vec_recv.at[base + mine],
            **device,
        )

    def vec_round(slots_ref, base, mine, size, device_of):
        others = [lax.rem(mine + step, size) for step in range(1, size)]
        for peer in others:
            vec_put(slots_ref, base, mine, peer, device_of(peer)).start()
        slots_ref[mine] = vectors[...]

        def finish():
            for peer in others:
                vec_put(slots_ref, base, mine, peer, device_of(peer)).wait_send()
                remote(
                    slots_ref.at[peer], slots_ref.at[peer],
                    vec_send.at[base + peer], vec_recv.at[base + peer], tensor=t,
                ).wait_recv()
            vectors[...] = total([slots_ref[index] for index in range(size)])

        return finish

    finish_vec = vec_round(vec_tensor, 0, t, ring, lambda peer: dict(tensor=peer))

    part_mix = part1
    gather_drain(1)
    def out_block(block, carry):
        cols = pl.ds(pl.multiple_of(block * local, local), local)
        part_mix[cols, 3 * local :] = dot(
            heads_side_by_side(context, slice(None)), g_all[:, cols], 0, 0
        ).astype(low)
        return carry

    lax.fori_loop(0, width // local, out_block, 0)

    def norm_again(s, carry):
        unit, _ = unit_rows(x_all[rows(s), :].astype(full))
        g_all[rows(s), :] = (unit * gain_one + shift_one).astype(low)
        return carry

    lax.fori_loop(0, ring, norm_again, 0)
    def mix_block(block, carry):
        span = pl.ds(pl.multiple_of(block * BLOCK, BLOCK), BLOCK)
        part_mix[span, 0 : 3 * local] = dot(
            g_all[:, span], grad_proj[:, 0 : 3 * local], 0, 0
        ).astype(low)
        return carry

    lax.fori_loop(0, width // BLOCK, mix_block, 0)
    mix_sum = DataSum(
        spots, (part_mix, done2, half2, a12, b12, a22, b22), data_send.at[2], data_recv.at[2]
    )
    mix_sum.stage(0)
    last_tick = (PIECES + 2) * ring - 6

    def ticks(share_from, share_to):
        u_steps(last_tick * share_from // 18, last_tick * share_to // 18)

    up_sum.stage(4)
    ticks(0, 11)
    mix_sum.stage(1)
    down_sum.stage(5)
    finish_vec()
    finish_vec = vec_round(
        vec_core, ring, core, 2, lambda peer: dict(dp=dp_of(peer, x_at, y_at))
    )
    ticks(11, 15)
    up_sum.stage(5)
    mix_sum.stage(2)
    finish_vec()
    finish_vec = vec_round(
        vec_x, ring + 2, x_at, nx, lambda peer: dict(dp=dp_of(core, peer, y_at))
    )
    down_sum.stage(6)
    copies = [pltpu.make_async_copy(done0, grad_down_out, out_sem.at[0])]
    copies[-1].start()
    ticks(15, 18)
    mix_sum.stage(3)
    up_sum.stage(6)
    copies.append(pltpu.make_async_copy(done1, grad_up_out, out_sem.at[1]))
    copies[-1].start()
    finish_vec()
    finish_vec = vec_round(
        vec_y, ring + 2 + nx, y_at, 2, lambda peer: dict(dp=dp_of(core, x_at, peer))
    )
    mix_sum.stage(4)
    branch_buf[t] = (x_all[rows(t), :].astype(full) + branch_own()).astype(low)
    copies.append(pltpu.make_async_copy(branch_buf.at[t], output_rows, out_sem.at[2]))
    copies[-1].start()
    own_cotangent = branch_buf.at[ring]
    own_load = pltpu.make_async_copy(cotangent, own_cotangent, load_sem.at[0])
    own_load.start()
    finish_vec()
    rows_all = group * ranks
    rms_active = jnp.sqrt(jnp.sum(vectors[4:5, :], axis=1, keepdims=True) / (rows_all * FF))
    rms_context = jnp.sqrt(jnp.sum(vectors[5:6, :], axis=1, keepdims=True) / (rows_all * width))
    vectors_out[0:4, :] = vectors[0:4, :]
    vectors_out[4:5, :] = jnp.broadcast_to(rms_context, (1, vectors.shape[1]))
    vectors_out[5:6, :] = jnp.broadcast_to(rms_active, (1, vectors.shape[1]))
    vectors_out[6:8, :] = jnp.zeros_like(vectors_out[6:8, :])
    weighted = u_own()
    own_load.wait()
    unit, scale = unit_rows(x_all[rows(t), :].astype(full))
    grad_rows = scale * (
        weighted
        - jnp.mean(weighted, axis=-1, keepdims=True)
        - unit * jnp.mean(weighted * unit, axis=-1, keepdims=True)
    )
    grad_buf[t] = (own_cotangent[...].astype(full) + grad_rows).astype(low)
    copies.append(pltpu.make_async_copy(grad_buf.at[t], input_grad, out_sem.at[3]))
    copies[-1].start()
    mix_sum.stage(5)
    mix_sum.stage(6)
    for part in range(3):
        copies.append(
            pltpu.make_async_copy(
                done2.at[:, part * local : (part + 1) * local],
                grad_qkv_out.at[part],
                out_sem.at[4 + part],
            )
        )
        copies[-1].start()
    for block in range(width // local):
        cols = slice(block * local, (block + 1) * local)
        copies.append(
            pltpu.make_async_copy(
                done2.at[cols, 3 * local :], grad_out_out.at[:, cols], out_sem.at[7 + block]
            )
        )
        copies[-1].start()
    gather_drain(0)
    branch_drain()
    u_drain()
    for copy in copies:
        copy.wait()


def widen_kernel(*refs):
    count = 6
    for source, target in zip(refs[:count], refs[count + 1 : 2 * count + 1]):
        target[...] = source[...].astype(target.dtype)
    vectors = refs[count]
    for index, target in enumerate(refs[2 * count + 1 :]):
        target[...] = vectors[index : index + 1, 0 : target.shape[1]]


def widen(arrays, vectors, width):
    steps = 4

    def spec(shape):
        block = list(shape)
        block[-2] //= steps
        lead = (0,) * (len(shape) - 2)
        return pl.BlockSpec(tuple(block), lambda i, lead=lead: (*lead, i, 0))

    kinds = [low, low, full, full, full, full]
    small = [(1, width)] * 4 + [(1, 1)] * 2
    whole = lambda shape: pl.BlockSpec(shape, lambda i: (0, 0))
    return pl.pallas_call(
        widen_kernel,
        name="widen",
        grid=(steps,),
        out_shape=[jax.ShapeDtypeStruct(a.shape, kind) for a, kind in zip(arrays, kinds)]
        + [jax.ShapeDtypeStruct(shape, full) for shape in small],
        in_specs=[spec(a.shape) for a in arrays] + [whole(vectors.shape)],
        out_specs=[spec(a.shape) for a in arrays] + [whole(shape) for shape in small],
    )(*arrays, vectors)


def per_device(
    ring, ranks,
    tokens, segments, w_qkv, w_out, w_up, w_down,
    gain_one, shift_one, gain_two, shift_two, cotangent,
):
    shard, width = tokens.shape
    group = segments.shape[1]
    local = w_qkv.shape[2]
    heads = local // HS
    hidden_local = w_up.shape[1]
    nx = ranks // 4
    half_rot = ROT // 2
    lane = np.arange(LANES) % HS
    frequency = rotary_base ** (-(2.0 * (lane % half_rot)) / ROT)
    frequency = np.where(lane < ROT, frequency, 0.0)
    sign = np.where(lane < half_rot, -1.0, 1.0)
    table = jnp.asarray(np.stack([frequency, sign] + [np.zeros(LANES)] * 6), jnp.float32)
    vmem = pl.BlockSpec(memory_space=pltpu.VMEM)
    anywhere = pl.BlockSpec(memory_space=pl.ANY)
    wide = max(width, hidden_local)
    scratch = lambda *shape: pltpu.VMEM(shape, low)
    wider = lambda *shape: pltpu.VMEM(shape, full)
    sems = lambda *shape: pltpu.SemaphoreType.DMA(shape)

    def sum_buffers(rows, columns):
        return [
            scratch(rows, columns),
            scratch(rows, columns),
            scratch(rows // 2, columns),
            scratch(nx - 1, rows // (4 * nx), columns),
            scratch(1, rows // 8, columns),
            scratch(1, rows // (8 * nx), columns),
            scratch(nx - 1, rows // (8 * nx), columns),
        ]

    data_sems = 12 + 4 * nx
    outs = pl.pallas_call(
        partial(layer_kernel, ring, ranks),
        name="layer",
        out_shape=[
            jax.ShapeDtypeStruct((shard, width), low),
            jax.ShapeDtypeStruct((shard, width), low),
            jax.ShapeDtypeStruct((hidden_local, width), low),
            jax.ShapeDtypeStruct((width, hidden_local), low),
            jax.ShapeDtypeStruct((3, width, local), low),
            jax.ShapeDtypeStruct((local, width), low),
            jax.ShapeDtypeStruct((8, wide), full),
        ],
        in_specs=[anywhere] * 2 + [vmem] * 6 + [anywhere] * 4,
        out_specs=[anywhere] * 6 + [vmem],
        scratch_shapes=[
            scratch(width, 3 * local), scratch(local, width),
            scratch(width, hidden_local), scratch(hidden_local, width),
            sems(8), sems(7 + width // local),
            wider(group, 1),
            scratch(group, width), scratch(group, width), scratch(group, width),
            scratch(group, hidden_local),
            wider(hidden_local // LANES, group, LANES),
            wider(group, width),
            wider(hidden_local, width), wider(width, hidden_local),
            scratch(heads, group, HS), scratch(heads, group, HS), scratch(heads, group, HS),
            scratch(heads, group, HS), scratch(heads, group, HS),
            wider(heads, 1, group),
            wider(heads, BLOCK, HS),
            wider(group, LANES), wider(group, LANES),
            sems(2, 2, ring), sems(2, ring),
            scratch(ring + 1, shard, width), sems(ring), sems(ring + 1),
            scratch(ring + 1, shard, width), sems(ring, PIECES), sems(ring + 1, PIECES),
            *sum_buffers(hidden_local, width),
            *sum_buffers(width, hidden_local)[1:],
            *sum_buffers(width, 4 * local)[1:],
            sems(3, data_sems), sems(3, data_sems),
            wider(8, wide), wider(ring, 8, wide), wider(2, 8, wide),
            wider(nx, 8, wide), wider(2, 8, wide),
            sems(ring + 4 + nx), sems(ring + 4 + nx),
        ],
        compiler_params=pltpu.CompilerParams(
            collective_id=0, has_side_effects=True, vmem_limit_bytes=67043328
        ),
    )(
        tokens, cotangent, segments,
        *(v.reshape(1, width) for v in (gain_one, shift_one, gain_two, shift_two)), table,
        w_qkv.transpose(1, 0, 2), w_out, w_up, w_down,
    )
    output_rows, input_grad, grad_down, grad_up, grad_qkv, grad_out, *small = widen(
        outs[:6], outs[6], width
    )
    return (
        output_rows,
        input_grad,
        grad_qkv.transpose(1, 0, 2),
        grad_out,
        grad_up,
        grad_down,
        *(v.reshape(width) for v in small[:4]),
        small[4].reshape(()),
        small[5].reshape(()),
    )


def solution(mesh):
    everyone = P(("dp", "tensor"), None)
    return jax.shard_map(
        partial(per_device, mesh.shape["tensor"], mesh.shape["dp"]),
        mesh=mesh,
        in_specs=(
            everyone,
            P("dp", None),
            P(None, None, "tensor"),
            P("tensor", None),
            P(None, "tensor"),
            P("tensor", None),
            P(),
            P(),
            P(),
            P(),
            everyone,
        ),
        out_specs=(
            everyone,
            everyone,
            P(None, None, "tensor"),
            P("tensor", None),
            P(None, "tensor"),
            P("tensor", None),
            P(),
            P(),
            P(),
            P(),
            P(),
            P(),
        ),
        check_vma=False,
    )
```
